32 devices in a mesh: gx: 4 (over y, x), gy: 4 (over z), gz: 2 (over core).
Axes of the slice: x: 2, y: 2, z: 4, core: 2. Of those that a mesh axis runs over, the one named last changes fastest.
Arguments:
- labels: int32 [16, 32], P('gx', 'gy'), may hold values from 0 to 2
- phase_noise: float32 [4, 16, 32, 256], P(None, 'gx', 'gy', 'gz'), may hold values from 0.05 to 0.6
- potentials: float32 [2, 16, 32, 256], P(None, 'gx', 'gy', 'gz'), may hold values from -3 to 3
- frame_shift: int32 [2], replicated, may hold values from 1 to 8, as said below
Outputs:
- final_phases: float32 [4, 16, 32, 256], P(None, 'gx', 'gy', 'gz')
- final_potentials: float32 [2, 16, 32, 256], P(None, 'gx', 'gy', 'gz')
The draws below stay inside these ranges and needn't reach their ends.
Inputs may be any that keep to these rules, and one draw needn't show every extreme that they name: `frame_shift`: each entry lies from 1 to 8, and at least one entry equals 8.
All inputs are finite; a program needn't handle non-finite values.
Results may differ from the reference program's by a relative error of at most 0.0001.
Values sent between devices are 32-bit elements; how exact they have to be, the bound alone decides.
A program may use at most 64 MiB of HBM per device.

```python
import math
import jax
import jax.numpy as jnp
from jax import lax

STEPS = 4
SHIFT_MAX = 8
NX = 16
NY = 32
NZ = 256


def draw_frame_shift(key, part):
    key_order, key_value = jax.random.split(jax.random.fold_in(key, 17))
    drawn_value = jax.random.randint(key_value, (1,), 1, SHIFT_MAX + 1).astype(jnp.int32)
    order_bit = jax.random.randint(key_order, (1,), 0, 2)
    largest = jnp.full((1,), SHIFT_MAX, jnp.int32)
    return jnp.where(order_bit == 0, jnp.concatenate([largest, drawn_value]), jnp.concatenate([drawn_value, largest]))


def place_ends(array, rng, low, high):
    extent = array.shape
    place = [jax.random.randint(jax.random.fold_in(rng, axis), (), 0, extent[axis]) for axis in range(len(extent))]
    array = array.at[tuple(place)].set(low)
    longest = extent.index(max(extent))
    place[longest] = (place[longest] + 1) % extent[longest]
    return array.at[tuple(place)].set(high)


def shard_levels(stream_key, extent, cuts, smallest, top_value):
    def one(axis_at, shards_of):
        draws = jax.random.uniform(jax.random.fold_in(jax.random.fold_in(stream_key, 6), axis_at), (shards_of,), jnp.float32, smallest / len(cuts), top_value / len(cuts))
        return jnp.repeat(jnp.exp(draws), extent[axis_at] // shards_of).reshape((-1,) + (1,) * (len(extent) - axis_at - 1))

    factor_of = one(*cuts[0])
    for cut in cuts[1:]:
        factor_of = factor_of * one(*cut)
    return factor_of


def scatter_about(own_key, extent, spread, limit, cuts=(), held_as=jnp.bfloat16):
    result = spread * jax.random.normal(own_key, extent, jnp.float32)
    if cuts:
        result = result * shard_levels(own_key, extent, cuts, -0.22, 0.18)
    return jnp.clip(result, -limit, limit).astype(held_as)


def setup_inputs(seed: int = 0) -> dict:
    splits = jax.random.split(jax.random.key(seed), 5)
    labels = place_ends(jax.random.randint(splits[0], (NX, NY), 0, 3), jax.random.fold_in(splits[0], 1), 0, 2).astype(jnp.int32)
    phase_noise = jnp.clip(0.05 + 0.55 * jax.random.uniform(splits[1], (4, NX, NY, NZ), jnp.float32) ** shard_levels(splits[1], (4, NX, NY, NZ), ((1, 4), (2, 4), (3, 2)), -0.2, 0.2), 0.05, 0.6)
    potentials = scatter_about(splits[2], (2, NX, NY, NZ), 0.5, 3.0, ((1, 4), (2, 4), (3, 2)), jnp.float32)
    frame_shift = draw_frame_shift(jax.random.fold_in(splits[4], 71), 0)
    return {"labels": labels, "phase_noise": phase_noise, "potentials": potentials, "frame_shift": frame_shift}


interface_width = 4.0
relax_time = 1.0
time_step = 0.12
obstacle_coef = 16.0 / (math.pi * math.pi)
normal_floor = 0.25
surface_table = [[0.0, 1.0, 1.2, 0.9], [1.0, 0.0, 1.1, 1.0], [1.2, 1.1, 0.0, 0.8], [0.9, 1.0, 0.8, 0.0]]
compositions = [[0.8, 0.1], [0.1, 0.8], [0.1, 0.1], [0.33, 0.33]]
latent_heat = [1.0, 0.9, 1.1, 0.0]
mobility_solid = 0.1
mobility_liquid = 1.0
trapping_coef = math.pi * 4.0 / 4.0
undercool_span = 2.0

def laplacian(padded):
    center = padded[:, 1:-1, 1:-1, 1:-1]
    total = padded[:, 2:, 1:-1, 1:-1] + padded[:, :-2, 1:-1, 1:-1]
    total = total + padded[:, 1:-1, 2:, 1:-1] + padded[:, 1:-1, :-2, 1:-1]
    total = total + padded[:, 1:-1, 1:-1, 2:] + padded[:, 1:-1, 1:-1, :-2]
    return total - 6.0 * center

def gradient(padded):
    along_x = 0.5 * (padded[:, 2:, 1:-1, 1:-1] - padded[:, :-2, 1:-1, 1:-1])
    along_y = 0.5 * (padded[:, 1:-1, 2:, 1:-1] - padded[:, 1:-1, :-2, 1:-1])
    along_z = 0.5 * (padded[:, 1:-1, 1:-1, 2:] - padded[:, 1:-1, 1:-1, :-2])
    return (along_x, along_y, along_z)

def phase_part(padded_phase, chem_pot, undercool):
    interior = padded_phase[:, 1:-1, 1:-1, 1:-1]
    curve = laplacian(padded_phase)
    drive_list = []
    for a in range(4):
        bend = jnp.zeros_like(interior[0])
        contact = jnp.zeros_like(interior[0])
        for b in range(4):
            if b != a:
                bend = bend + surface_table[a][b] * (interior[b] * curve[a] - interior[a] * curve[b])
                contact = contact + surface_table[a][b] * interior[b]
        variation = -interface_width * bend + obstacle_coef / interface_width * contact
        variation = variation - (compositions[a][0] * chem_pot[0] + compositions[a][1] * chem_pot[1])
        variation = variation + latent_heat[a] * undercool
        drive_list.append(variation)
    variation = jnp.stack(drive_list)
    average = lax.optimization_barrier(jnp.mean(variation, axis=0))
    growth_rate = -(variation - average) / (relax_time * interface_width)
    clipped = jnp.clip(interior + time_step * growth_rate, 0.0, 1.0)
    updated = clipped / lax.optimization_barrier(jnp.sum(clipped, axis=0))
    change = (updated - interior) / time_step
    slopes = gradient(padded_phase)
    magnitude = jnp.sqrt(slopes[0] * slopes[0] + slopes[1] * slopes[1] + slopes[2] * slopes[2])
    inverse_norm = 1.0 / jnp.maximum(magnitude, normal_floor)
    carried = [4.0 * interior[a] * interior[3] * change[a] * inverse_norm[a] for a in range(3)]
    currents = []
    for k in range(2):
        for d in range(3):
            total = jnp.zeros_like(interior[0])
            for a in range(3):
                total = total + (compositions[3][k] - compositions[a][k]) * carried[a] * slopes[d][a]
            currents.append(-trapping_coef * total)
    return (updated, change, jnp.stack(currents))

def neighbor(block, d, offset):
    pieces = [slice(1, -1), slice(1, -1), slice(1, -1)]
    pieces[d] = slice(1 + offset, block.shape[d] - 1 + offset)
    return block[tuple(pieces)]

def potential_part(padded_pot, padded_mob, padded_flux, change):
    center_mob = padded_mob[1:-1, 1:-1, 1:-1]
    results = []
    for k in range(2):
        chem = padded_pot[k]
        center = chem[1:-1, 1:-1, 1:-1]
        divergence = jnp.zeros_like(center)
        for d in range(3):
            current = padded_flux[3 * k + d]
            upper_face = 0.5 * (neighbor(padded_mob, d, 1) + center_mob) * (neighbor(chem, d, 1) - center)
            upper_face = upper_face - 0.5 * (neighbor(current, d, 1) + neighbor(current, d, 0))
            lower_face = 0.5 * (center_mob + neighbor(padded_mob, d, -1)) * (center - neighbor(chem, d, -1))
            lower_face = lower_face - 0.5 * (neighbor(current, d, 0) + neighbor(current, d, -1))
            divergence = divergence + (upper_face - lower_face)
        source = jnp.zeros_like(center)
        for a in range(4):
            source = source + compositions[a][k] * change[a]
        results.append(center + time_step * (divergence - source))
    return jnp.stack(results)

def pad_field(block):
    block = jnp.pad(block, ((0, 0), (1, 1), (1, 1), (0, 0)), mode='wrap')
    return jnp.pad(block, ((0, 0), (0, 0), (0, 0), (1, 1)), mode='edge')

def reference(labels, phase_noise, potentials, frame_shift):
    zindex = jnp.arange(NZ, dtype=jnp.int32)
    zpos = zindex.astype(jnp.float32)
    undercool = undercool_span * (zpos + 0.5 - NZ // 2) / NZ
    solid = zindex < NZ // 2
    onehot = []
    for a in range(3):
        onehot.append(((labels == a)[:, :, None] & solid[None, None, :]).astype(jnp.float32))
    onehot.append(jnp.broadcast_to((~solid)[None, None, :], (NX, NY, NZ)).astype(jnp.float32))
    initial = jnp.stack(onehot) + phase_noise
    phases = initial / lax.optimization_barrier(jnp.sum(initial, axis=0))
    fields = jnp.concatenate([phases, potentials], axis=0)
    for step_index in range(STEPS):
        padded = pad_field(fields)
        phases_new, change, currents = phase_part(padded[:4], fields[4:], undercool)
        currents = pad_field(currents)
        mobility = mobility_solid + (mobility_liquid - mobility_solid) * padded[3]
        chem_new = potential_part(padded[4:], mobility, currents, change)
        fields = jnp.concatenate([phases_new, chem_new], axis=0)
        if step_index % 2 == 0:
            far = jnp.concatenate([jnp.zeros((3, NX, NY, SHIFT_MAX), jnp.float32), jnp.ones((1, NX, NY, SHIFT_MAX), jnp.float32), jnp.zeros((2, NX, NY, SHIFT_MAX), jnp.float32)], axis=0)
            joined = jnp.concatenate([fields, far], axis=3)
            offset = frame_shift[step_index // 2].astype(jnp.int32)
            fields = lax.dynamic_slice_in_dim(joined, offset, NZ, axis=3)
    return (fields[:4], fields[4:])
```

```python
import functools
import math

import jax
import jax.numpy as jnp
from jax import lax
from jax.experimental import pallas as pl
from jax.experimental.pallas import tpu as pltpu
from jax.sharding import PartitionSpec as P

MESH = pl.DeviceIdType.MESH
STEPS = 4

interface_width = 4.0
time_step = 0.12
obstacle_coef = 16.0 / (math.pi * math.pi)
normal_floor = 0.25
surface_table = [
    [0.0, 1.0, 1.2, 0.9],
    [1.0, 0.0, 1.1, 1.0],
    [1.2, 1.1, 0.0, 0.8],
    [0.9, 1.0, 0.8, 0.0],
]
compositions = [[0.8, 0.1], [0.1, 0.8], [0.1, 0.1], [0.33, 0.33]]
latent_heat = [1.0, 0.9, 1.1, 0.0]
trapping_coef = math.pi * 4.0 / 4.0
undercool_span = 2.0

OWN, YH, ZH, YZ = 0, 1, 2, 3


def phase_update(center, nb, m, theta):
    lap = []
    for a in range(3):
        total = (nb[0][0][a] + nb[0][1][a]) + (nb[1][0][a] + nb[1][1][a])
        total = total + (nb[2][0][a] + nb[2][1][a])
        lap.append(total - 6.0 * center[a])
    lap.append(-(lap[0] + lap[1] + lap[2]))
    p = list(center) + [1.0 - (center[0] + center[1] + center[2])]

    def weigh(f, a):
        terms = [f[b] if surface_table[a][b] == 1.0 else surface_table[a][b] * f[b] for b in range(4) if b != a]
        return terms[0] + terms[1] + terms[2]

    drive = []
    for a in range(4):
        gp = weigh(p, a)
        gl = weigh(lap, a)
        v = gp * (obstacle_coef / interface_width - interface_width * lap[a]) + (interface_width * p[a]) * gl
        v = v - (compositions[a][0] * m[0] + compositions[a][1] * m[1])
        if latent_heat[a]:
            v = v + latent_heat[a] * theta
        drive.append(v)
    mean = 0.25 * ((drive[0] + drive[1]) + (drive[2] + drive[3]))
    q = [jnp.clip(p[a] - (time_step / interface_width) * (drive[a] - mean), 0.0, 1.0) for a in range(4)]
    inv = 1.0 / ((q[0] + q[1]) + (q[2] + q[3]))
    new = [q[a] * inv for a in range(4)]
    rate = [(new[a] - p[a]) * (1.0 / time_step) for a in range(4)]
    return p, new, rate


def carried_part(p, rate, nb):
    p3 = p[3] * 4.0
    carried, slopes = [], []
    for a in range(3):
        g = [0.5 * (nb[d][1][a] - nb[d][0][a]) for d in range(3)]
        square = g[0] * g[0] + g[1] * g[1] + g[2] * g[2]
        inv = lax.rsqrt(jnp.maximum(square, normal_floor * normal_floor))
        carried.append(p[a] * p3 * rate[a] * inv)
        slopes.append(g)
    return carried, slopes


def current(carried, slopes, d):
    out = []
    for k in range(2):
        total = None
        for a in range(3):
            term = (-trapping_coef * (compositions[3][k] - compositions[a][k])) * (carried[a] * slopes[a][d])
            total = term if total is None else total + term
        out.append(total)
    return out


def kernel(labels_ref, noise_ref, pot_ref, shift_ref, phase_out, pot_out,
           S, W, zrcv, ysnd, yrcv, csnd, crcv, send_sem, recv_sem):
    rows, ny, nl = noise_ref.shape[1:]
    gx, gy, gz = lax.axis_index("gx"), lax.axis_index("gy"), lax.axis_index("gz")
    nx_dev, ny_dev, nz_dev = lax.axis_size("gx"), lax.axis_size("gy"), lax.axis_size("gz")

    def near(index, count, step):
        return lax.rem(index + (count + step), count)

    xs = {-1: near(gx, nx_dev, -1), 1: near(gx, nx_dev, 1)}
    ys = {-1: near(gy, ny_dev, -1), 1: near(gy, ny_dev, 1)}
    zs = {-1: near(gz, nz_dev, -1), 1: near(gz, nz_dev, 1)}
    corners = [(-1, -1), (-1, 1), (1, -1), (1, 1)]
    targets = [{"gz": zs[-1]}, {"gz": zs[1]}, {"gx": xs[-1]}, {"gx": xs[1]}, {"gy": ys[-1]}, {"gy": ys[1]}]
    targets += [{"gx": xs[i], "gy": ys[j]} for i, j in corners]

    barrier = pltpu.get_barrier_semaphore()
    for target in targets:
        pl.semaphore_signal(barrier, inc=1, device_id=target, device_id_type=MESH)

    lane = lax.broadcasted_iota(jnp.int32, (ny, nl), 1)
    row = lax.broadcasted_iota(jnp.int32, (ny, nl), 0)
    lower = gz == 0
    upper = gz == nz_dev - 1
    total_planes = nl * nz_dev
    front = total_planes // 2
    zown = gz * nl + lane
    zhalo = jnp.where(lane < nl // 2, zown + nl, zown - nl)

    def theta_of(index):
        return undercool_span * (index.astype(jnp.float32) + 0.5 - front) / total_planes

    theta = {OWN: theta_of(zown), ZH: theta_of(zhalo)}
    theta[YH] = theta[OWN]
    solid = zown < front

    def up_y(a, b):
        return pltpu.roll(jnp.where(row == 0, b, a), ny - 1, 0)

    def down_y(a, b):
        return pltpu.roll(jnp.where(row == ny - 1, b, a), 1, 0)

    def up_z(a, b):
        return pltpu.roll(jnp.where(lane == 0, b, a), nl - 1, 1)

    def down_z(a, b):
        return pltpu.roll(jnp.where(lane == nl - 1, b, a), 1, 1)

    lrow = lax.broadcasted_iota(jnp.int32, (ny, ny), 0)
    lcol = lax.broadcasted_iota(jnp.int32, (ny, ny), 1)
    for x in range(rows):
        lab = jnp.broadcast_to(labels_ref[x : x + 1, :].astype(jnp.float32), (ny, ny))
        lab = jnp.sum(jnp.where(lrow == lcol, lab, 0.0), axis=1, keepdims=True)
        lab = jnp.broadcast_to(lab, (ny, nl))
        init = []
        for a in range(3):
            init.append(noise_ref[a, x] + jnp.where((lab == float(a)) & solid, 1.0, 0.0))
        init.append(noise_ref[3, x] + jnp.where(solid, 0.0, 1.0))
        inv = 1.0 / ((init[0] + init[1]) + (init[2] + init[3]))
        for a in range(3):
            S[0, a, x] = init[a] * inv
        for k in range(2):
            S[0, 3 + k, x] = pot_ref[k, x]

    pl.semaphore_wait(barrier, len(targets))

    def step(t, carry):
        def copy(src, dst, n, target):
            return pltpu.make_async_remote_copy(
                src_ref=src, dst_ref=dst, send_sem=send_sem.at[t, n], recv_sem=recv_sem.at[t, n],
                device_id=target, device_id_type=MESH,
            )

        zcopies = [
            copy(S.at[t], zrcv.at[t, 0], 0, {"gz": zs[1]}),
            copy(S.at[t], zrcv.at[t, 1], 1, {"gz": zs[-1]}),
        ]
        for c in zcopies:
            c.start()
        for c in zcopies:
            c.wait_recv()
        shift = shift_ref[t]
        bits = [(shift & 1) != 0, (shift & 2) != 0, (shift & 4) != 0, (shift & 8) != 0]
        for x in range(rows):
            for f in range(5):
                own = S[t, f, x]
                above = jnp.where(upper, 0.0, zrcv[t, 1, f, x])
                halo = jnp.where(lane < nl // 2, above, zrcv[t, 0, f, x])
                for bit in range(4):
                    by = 1 << bit
                    mixed_own = jnp.where(lane < by, halo, own)
                    mixed_halo = jnp.where(lane < by, own, halo)
                    own = jnp.where(bits[bit], pltpu.roll(mixed_own, nl - by, 1), own)
                    halo = jnp.where(bits[bit], pltpu.roll(mixed_halo, nl - by, 1), halo)
                first = jnp.broadcast_to(own[:, 0:1], (ny, nl))
                last = jnp.broadcast_to(own[:, nl - 1 : nl], (ny, nl))
                halo = jnp.where(upper & (lane < nl // 2), last, halo)
                halo = jnp.where(lower & (lane >= nl // 2), first, halo)
                W[t, f, x + 2, OWN] = own
                W[t, f, x + 2, ZH] = halo
                if f < 3:
                    ysnd[t, 0, f, 2 * x : 2 * x + 2, :] = own[0:2]
                    ysnd[t, 1, f, 2 * x : 2 * x + 2, :] = own[ny - 2 : ny]
                    at = f * rows + x
                    ysnd[t, 0, 4 + at // ny, at % ny : at % ny + 1, :] = halo[0:1]
                    ysnd[t, 1, 4 + at // ny, at % ny : at % ny + 1, :] = halo[ny - 1 : ny]
                    for n, (i, j) in enumerate(corners):
                        if x == (0 if i < 0 else rows - 1):
                            csnd[t, n, f : f + 1, :] = own[0:1] if j < 0 else own[ny - 1 : ny]
                else:
                    at = (f - 3) * rows + x
                    ysnd[t, 0, 3, at : at + 1, :] = own[0:1]
                    ysnd[t, 1, 3, at : at + 1, :] = own[ny - 1 : ny]

        copies = []
        for n, (i, j) in enumerate(corners):
            copies.append(copy(csnd.at[t, n], crcv.at[t, n], 2 + n, {"gx": xs[i], "gy": ys[j]}))
        low, high = (2, rows + 2), (rows, 0)
        for side, (src, dst) in ((-1, low), (1, high)):
            base = 6 + (0 if side < 0 else 3)
            edge_src = 2 if side < 0 else rows + 1
            edge_dst = rows + 2 if side < 0 else 1
            target = {"gx": xs[side]}
            copies.append(copy(W.at[t, pl.ds(0, 3), pl.ds(src, 2), OWN], W.at[t, pl.ds(0, 3), pl.ds(dst, 2), OWN], base, target))
            copies.append(copy(W.at[t, pl.ds(3, 2), edge_src, OWN], W.at[t, pl.ds(3, 2), edge_dst, OWN], base + 1, target))
            copies.append(copy(W.at[t, pl.ds(0, 3), edge_src, ZH], W.at[t, pl.ds(0, 3), edge_dst, ZH], base + 2, target))
        copies.append(copy(ysnd.at[t, 0], yrcv.at[t, 0], 12, {"gy": ys[-1]}))
        copies.append(copy(ysnd.at[t, 1], yrcv.at[t, 1], 13, {"gy": ys[1]}))
        for c in copies:
            c.start()
        for c in copies:
            c.wait_recv()

        for x in range(rows):
            for f in range(3):
                W[t, f, x + 2, YH, 0:2, :] = yrcv[t, 0, f, 2 * x : 2 * x + 2, :]
                W[t, f, x + 2, YH, ny - 2 : ny, :] = yrcv[t, 1, f, 2 * x : 2 * x + 2, :]
                at = f * rows + x
                W[t, f, x + 2, YZ, 0:1, :] = yrcv[t, 0, 4 + at // ny, at % ny : at % ny + 1, :]
                W[t, f, x + 2, YZ, ny - 1 : ny, :] = yrcv[t, 1, 4 + at // ny, at % ny : at % ny + 1, :]
            for k in range(2):
                at = k * rows + x
                W[t, 3 + k, x + 2, YH, 0:1, :] = yrcv[t, 0, 3, at : at + 1, :]
                W[t, 3 + k, x + 2, YH, ny - 1 : ny, :] = yrcv[t, 1, 3, at : at + 1, :]
        for n, (i, j) in enumerate(corners):
            xdst = rows + 2 if i < 0 else 1
            ydst = 0 if j < 0 else ny - 1
            for f in range(3):
                W[t, f, xdst, YH, ydst : ydst + 1, :] = crcv[t, n, f : f + 1, :]

        def field(x, q, fs=(0, 1, 2)):
            return [W[t, f, x, q] for f in fs]

        partner_y = {OWN: YH, YH: OWN, ZH: YZ}
        partner_z = {OWN: ZH, ZH: OWN, YH: YZ}

        def neighbours(x, q, fs=(0, 1, 2), with_x=True):
            c = field(x, q, fs)
            py = field(x, partner_y[q], fs)
            pz = field(x, partner_z[q], fs)
            n = len(fs)
            return c, [
                (field(x - 1, q, fs), field(x + 1, q, fs)),
                ([down_y(c[a], py[a]) for a in range(n)], [up_y(c[a], py[a]) for a in range(n)]),
                ([down_z(c[a], pz[a]) for a in range(n)], [up_z(c[a], pz[a]) for a in range(n)]),
            ]

        jx = {}
        partial = {}
        for x in range(1, rows + 3):
            inside = 2 <= x < rows + 2
            m = field(x, OWN, (3, 4))
            c, nb = neighbours(x, OWN)
            p, new, rate = phase_update(c, nb, m, theta[OWN])
            carried, slopes = carried_part(p, rate, nb)
            jx[x] = current(carried, slopes, 0)
            if inside:
                for a in range(3):
                    S[t + 1, a, x - 2] = new[a]
                phase_out[3, x - 2] = new[3]
                _, mb = neighbours(x, OWN, (3, 4))
                diff = [None, None]
                s = (c[0] + c[1]) + c[2]
                for d in range(3):
                    for side in range(2):
                        around = nb[d][side]
                        mob = 1.0 - 0.45 * (((around[0] + around[1]) + around[2]) + s)
                        for k in range(2):
                            flow = mob * (mb[d][side][k] - m[k])
                            diff[k] = flow if diff[k] is None else diff[k] + flow
                for k in range(2):
                    for a in range(4):
                        diff[k] = diff[k] - compositions[a][k] * rate[a]
                jy = current(carried, slopes, 1)
                jz = current(carried, slopes, 2)
                cb, nbb = neighbours(x, YH)
                pb, _, rb = phase_update(cb, nbb, field(x, YH, (3, 4)), theta[YH])
                jyb = current(*carried_part(pb, rb, nbb), 1)
                cz, nbz = neighbours(x, ZH)
                pz, _, rz = phase_update(cz, nbz, field(x, ZH, (3, 4)), theta[ZH])
                jzb = current(*carried_part(pz, rz, nbz), 2)
                for k in range(2):
                    dy = up_y(jy[k], jyb[k]) - down_y(jy[k], jyb[k])
                    above = jnp.where(upper & (lane == nl - 1), jz[k], up_z(jz[k], jzb[k]))
                    below = jnp.where(lower & (lane == 0), jz[k], down_z(jz[k], jzb[k]))
                    diff[k] = diff[k] - 0.5 * (dy + (above - below))
                partial[x] = (m, diff)
            if x >= 3:
                at = x - 1
                if 2 <= at < rows + 2:
                    m_at, diff_at = partial.pop(at)
                    for k in range(2):
                        total = diff_at[k] - 0.5 * (jx[at + 1][k] - jx[at - 1][k])
                        S[t + 1, 3 + k, at - 2] = m_at[k] + time_step * total
        for c in zcopies + copies:
            c.wait_send()
        return carry

    lax.fori_loop(0, STEPS, step, 0)
    for a in range(3):
        phase_out[a] = S[STEPS, a]
    for k in range(2):
        pot_out[k] = S[STEPS, 3 + k]


def on_device(labels, phase_noise, potentials, frame_shift):
    _, rows, ny, nl = phase_noise.shape
    none = jnp.zeros((1,), jnp.int32)
    shifts = jnp.concatenate([none, frame_shift[0:1], none, frame_shift[1:2]])
    shifts = jnp.broadcast_to(shifts[:, None, None], (STEPS, ny, nl))
    vmem = pl.BlockSpec(memory_space=pltpu.VMEM)
    f32 = jnp.float32
    return pl.pallas_call(
        kernel,
        out_shape=(
            jax.ShapeDtypeStruct(phase_noise.shape, f32),
            jax.ShapeDtypeStruct(potentials.shape, f32),
        ),
        in_specs=[vmem] * 4,
        out_specs=(vmem, vmem),
        scratch_shapes=[
            pltpu.VMEM((STEPS + 1, 5, rows, ny, nl), f32),
            pltpu.VMEM((STEPS, 5, rows + 4, 4, ny, nl), f32),
            pltpu.VMEM((STEPS, 2, 5, rows, ny, nl), f32),
            pltpu.VMEM((STEPS, 2, 6, ny, nl), f32),
            pltpu.VMEM((STEPS, 2, 6, ny, nl), f32),
            pltpu.VMEM((STEPS, 4, ny, nl), f32),
            pltpu.VMEM((STEPS, 4, ny, nl), f32),
            pltpu.SemaphoreType.DMA((STEPS, 14)),
            pltpu.SemaphoreType.DMA((STEPS, 14)),
        ],
        compiler_params=pltpu.CompilerParams(collective_id=0, has_side_effects=True),
        name="eutectic",
    )(labels, phase_noise, potentials, shifts)


def solution(mesh):
    placed = (P("gx", "gy"), P(None, "gx", "gy", "gz"), P(None, "gx", "gy", "gz"), P())
    return jax.shard_map(
        on_device,
        mesh=mesh,
        in_specs=placed,
        out_specs=(P(None, "gx", "gy", "gz"), P(None, "gx", "gy", "gz")),
        check_vma=False,
    )
```

```python
import functools
import math

import jax
import jax.numpy as jnp
from jax import lax
from jax.experimental import pallas as pl
from jax.experimental.pallas import tpu as pltpu
from jax.sharding import PartitionSpec as P

MESH = pl.DeviceIdType.MESH
STEPS = 4

interface_width = 4.0
time_step = 0.12
obstacle_coef = 16.0 / (math.pi * math.pi)
normal_floor = 0.25
surface_table = [
    [0.0, 1.0, 1.2, 0.9],
    [1.0, 0.0, 1.1, 1.0],
    [1.2, 1.1, 0.0, 0.8],
    [0.9, 1.0, 0.8, 0.0],
]
compositions = [[0.8, 0.1], [0.1, 0.8], [0.1, 0.1], [0.33, 0.33]]
latent_heat = [1.0, 0.9, 1.1, 0.0]
trapping_coef = math.pi * 4.0 / 4.0
undercool_span = 2.0

OWN, YH, ZH, YZ = 0, 1, 2, 3


def phase_update(center, nb, m, theta):
    lap = []
    for a in range(3):
        total = (nb[0][0][a] + nb[0][1][a]) + (nb[1][0][a] + nb[1][1][a])
        total = total + (nb[2][0][a] + nb[2][1][a])
        lap.append(total - 6.0 * center[a])
    lap.append(-(lap[0] + lap[1] + lap[2]))
    p = list(center) + [1.0 - (center[0] + center[1] + center[2])]

    def weigh(f, a):
        terms = [f[b] if surface_table[a][b] == 1.0 else surface_table[a][b] * f[b] for b in range(4) if b != a]
        return terms[0] + terms[1] + terms[2]

    drive = []
    for a in range(4):
        gp = weigh(p, a)
        gl = weigh(lap, a)
        v = gp * (obstacle_coef / interface_width - interface_width * lap[a]) + (interface_width * p[a]) * gl
        v = v - (compositions[a][0] * m[0] + compositions[a][1] * m[1])
        if latent_heat[a]:
            v = v + latent_heat[a] * theta
        drive.append(v)
    mean = 0.25 * ((drive[0] + drive[1]) + (drive[2] + drive[3]))
    q = [jnp.clip(p[a] - (time_step / interface_width) * (drive[a] - mean), 0.0, 1.0) for a in range(4)]
    inv = 1.0 / ((q[0] + q[1]) + (q[2] + q[3]))
    new = [q[a] * inv for a in range(4)]
    rate = [(new[a] - p[a]) * (1.0 / time_step) for a in range(4)]
    return p, new, rate


def carried_part(p, rate, nb):
    p3 = p[3] * 4.0
    carried, slopes = [], []
    for a in range(3):
        g = [0.5 * (nb[d][1][a] - nb[d][0][a]) for d in range(3)]
        square = g[0] * g[0] + g[1] * g[1] + g[2] * g[2]
        inv = lax.rsqrt(jnp.maximum(square, normal_floor * normal_floor))
        carried.append(p[a] * p3 * rate[a] * inv)
        slopes.append(g)
    return carried, slopes


def current(carried, slopes, d):
    out = []
    for k in range(2):
        total = None
        for a in range(3):
            term = (-trapping_coef * (compositions[3][k] - compositions[a][k])) * (carried[a] * slopes[a][d])
            total = term if total is None else total + term
        out.append(total)
    return out


def kernel(labels_hbm, noise_hbm, pot_hbm, shift_hbm, phase_out, pot_out,
           labels_ref, noise_ref, pot_ref, shift_ref, in_sem,
           S, W, zrcv, ysnd, yrcv, yzsnd, yzrcv, xzsnd, xzrcv, csnd, crcv, send_sem, recv_sem):
    fetches = [
        pltpu.make_async_copy(src, dst, in_sem.at[n])
        for n, (src, dst) in enumerate(
            ((labels_hbm, labels_ref), (noise_hbm, noise_ref), (pot_hbm, pot_ref), (shift_hbm, shift_ref))
        )
    ]
    for fetch in fetches:
        fetch.start()
    rows, ny, nl = noise_ref.shape[1:]
    gx, gy, gz = lax.axis_index("gx"), lax.axis_index("gy"), lax.axis_index("gz")
    nx_dev, ny_dev, nz_dev = lax.axis_size("gx"), lax.axis_size("gy"), lax.axis_size("gz")

    def near(index, count, step):
        return lax.rem(index + (count + step), count)

    xs = {-1: near(gx, nx_dev, -1), 1: near(gx, nx_dev, 1)}
    ys = {-1: near(gy, ny_dev, -1), 1: near(gy, ny_dev, 1)}
    zs = {-1: near(gz, nz_dev, -1), 1: near(gz, nz_dev, 1)}
    corners = [(-1, -1), (-1, 1), (1, -1), (1, 1)]
    targets = [{"gx": xs[i], "gy": ys[j]} for i, j in corners]
    targets += [{"gx": xs[-1]}, {"gx": xs[1]}, {"gy": ys[-1]}, {"gy": ys[1]}, {"gz": zs[-1]}, {"gz": zs[1]}]

    barrier = pltpu.get_barrier_semaphore()
    for target in targets:
        pl.semaphore_signal(barrier, inc=1, device_id=target, device_id_type=MESH)

    lane = lax.broadcasted_iota(jnp.int32, (ny, nl), 1)
    row = lax.broadcasted_iota(jnp.int32, (ny, nl), 0)
    lower = gz == 0
    upper = gz == nz_dev - 1
    total_planes = nl * nz_dev
    front = total_planes // 2
    zown = gz * nl + lane
    zhalo = jnp.where(lane < nl // 2, zown + nl, zown - nl)

    def theta_of(index):
        return undercool_span * (index.astype(jnp.float32) + 0.5 - front) / total_planes

    theta = {OWN: theta_of(zown), ZH: theta_of(zhalo)}
    theta[YH] = theta[OWN]
    solid = zown < front

    def up_y(a, b):
        return pltpu.roll(jnp.where(row == 0, b, a), ny - 1, 0)

    def down_y(a, b):
        return pltpu.roll(jnp.where(row == ny - 1, b, a), 1, 0)

    def up_z(a, b):
        return pltpu.roll(jnp.where(lane == 0, b, a), nl - 1, 1)

    def down_z(a, b):
        return pltpu.roll(jnp.where(lane == nl - 1, b, a), 1, 1)

    for fetch in fetches:
        fetch.wait()
    first_shift, second_shift = shift_ref[0], shift_ref[1]
    lrow = lax.broadcasted_iota(jnp.int32, (ny, ny), 0)
    lcol = lax.broadcasted_iota(jnp.int32, (ny, ny), 1)
    for x in range(rows):
        lab = jnp.broadcast_to(labels_ref[x : x + 1, :].astype(jnp.float32), (ny, ny))
        lab = jnp.sum(jnp.where(lrow == lcol, lab, 0.0), axis=1, keepdims=True)
        lab = jnp.broadcast_to(lab, (ny, nl))
        init = []
        for a in range(3):
            init.append(noise_ref[a, x] + jnp.where((lab == float(a)) & solid, 1.0, 0.0))
        init.append(noise_ref[3, x] + jnp.where(solid, 0.0, 1.0))
        inv = 1.0 / ((init[0] + init[1]) + (init[2] + init[3]))
        for a in range(3):
            W[0, a, x + 2, OWN] = init[a] * inv
        for k in range(2):
            W[0, 3 + k, x + 2, OWN] = pot_ref[k, x]

    pl.semaphore_wait(barrier, len(targets))

    def step(t, shifted, store):
        def copy(src, dst, n, target):
            return pltpu.make_async_remote_copy(
                src_ref=src, dst_ref=dst, send_sem=send_sem.at[t, n], recv_sem=recv_sem.at[t, n],
                device_id=target, device_id_type=MESH,
            )

        block = S.at[t // 2] if shifted else W.at[t, pl.ds(0, 5), pl.ds(2, rows), OWN]
        zcopies = [
            copy(block, zrcv.at[t, 0], 0, {"gz": zs[1]}),
            copy(block, zrcv.at[t, 1], 1, {"gz": zs[-1]}),
        ]
        for c in zcopies:
            c.start()

        copies = []

        def launch(c):
            c.start()
            copies.append(c)

        def pack_own(x, f, own):
            if f < 3:
                ysnd[t, 0, f, 2 * x : 2 * x + 2, :] = own[0:2]
                ysnd[t, 1, f, 2 * x : 2 * x + 2, :] = own[ny - 2 : ny]
                for n, (i, j) in enumerate(corners):
                    if x == (0 if i < 0 else rows - 1):
                        csnd[t, n, f : f + 1, :] = own[0:1] if j < 0 else own[ny - 1 : ny]
            else:
                at = (f - 3) * rows + x
                ysnd[t, 0, 3, at : at + 1, :] = own[0:1]
                ysnd[t, 1, 3, at : at + 1, :] = own[ny - 1 : ny]

        def send_own():
            low, high = (2, rows + 2), (rows, 0)
            for side, (src, dst) in ((-1, low), (1, high)):
                base = 6 + (0 if side < 0 else 2)
                edge_src = 2 if side < 0 else rows + 1
                edge_dst = rows + 2 if side < 0 else 1
                target = {"gx": xs[side]}
                launch(copy(W.at[t, pl.ds(0, 3), pl.ds(src, 2), OWN], W.at[t, pl.ds(0, 3), pl.ds(dst, 2), OWN], base, target))
                launch(copy(W.at[t, pl.ds(3, 2), edge_src, OWN], W.at[t, pl.ds(3, 2), edge_dst, OWN], base + 1, target))

        def send_y():
            for n, (i, j) in enumerate(corners):
                launch(copy(csnd.at[t, n], crcv.at[t, n], 2 + n, {"gx": xs[i], "gy": ys[j]}))
            launch(copy(ysnd.at[t, 0], yrcv.at[t, 0], 10, {"gy": ys[-1]}))
            launch(copy(ysnd.at[t, 1], yrcv.at[t, 1], 11, {"gy": ys[1]}))

        if not shifted:
            send_own()
            for x in range(rows):
                for f in range(5):
                    pack_own(x, f, W[t, f, x + 2, OWN])
            send_y()
        for c in zcopies:
            c.wait_recv()
        if shifted:
            shift = jnp.full((ny, nl), jnp.where(t == 1, first_shift, second_shift), jnp.int32)
            bits = [(shift & 1) != 0, (shift & 2) != 0, (shift & 4) != 0, (shift & 8) != 0]
        packed = {}
        for x in range(rows):
            for f in range(5):
                own = S[t // 2, f, x] if shifted else W[t, f, x + 2, OWN]
                halo = jnp.where(lane < nl // 2, zrcv[t, 1, f, x], zrcv[t, 0, f, x])
                if shifted:
                    halo = jnp.where(upper & (lane < nl // 2), 0.0, halo)
                    for bit in range(4):
                        by = 1 << bit
                        mixed_own = jnp.where(lane < by, halo, own)
                        mixed_halo = jnp.where(lane < by, own, halo)
                        own = jnp.where(bits[bit], pltpu.roll(mixed_own, nl - by, 1), own)
                        halo = jnp.where(bits[bit], pltpu.roll(mixed_halo, nl - by, 1), halo)
                    W[t, f, x + 2, OWN] = own
                    pack_own(x, f, own)
                first = jnp.broadcast_to(own[:, 0:1], (ny, nl))
                last = jnp.broadcast_to(own[:, nl - 1 : nl], (ny, nl))
                halo = jnp.where(upper & (lane < nl // 2), last, halo)
                halo = jnp.where(lower & (lane >= nl // 2), first, halo)
                W[t, f, x + 2, ZH] = halo
                if f < 3:
                    at = f * rows + x
                    yzsnd[t, 0, at // ny, at % ny : at % ny + 1, :] = halo[0:1]
                    yzsnd[t, 1, at // ny, at % ny : at % ny + 1, :] = halo[ny - 1 : ny]
                    if x == 0 or x == rows - 1:
                        mixed = halo if f == 0 else jnp.where(
                            (lane == 8 * f) | (lane == 8 * f - 1), pltpu.roll(halo, 8 * f, 1), packed[x])
                        packed[x] = mixed
        xzsnd[t, 0] = packed[0]
        xzsnd[t, 1] = packed[rows - 1]
        if shifted:
            send_own()
            send_y()
        launch(copy(xzsnd.at[t, 0], xzrcv.at[t, 0], 12, {"gx": xs[-1]}))
        launch(copy(xzsnd.at[t, 1], xzrcv.at[t, 1], 13, {"gx": xs[1]}))
        launch(copy(yzsnd.at[t, 0], yzrcv.at[t, 0], 14, {"gy": ys[-1]}))
        launch(copy(yzsnd.at[t, 1], yzrcv.at[t, 1], 15, {"gy": ys[1]}))
        for c in copies:
            c.wait_recv()

        for f in range(3):
            by = 8 * f
            for slot, xdst in ((0, rows + 2), (1, 1)):
                halo = xzrcv[t, slot]
                W[t, f, xdst, ZH] = pltpu.roll(halo, nl - by, 1) if by else halo
        for x in range(rows):
            for f in range(3):
                W[t, f, x + 2, YH, 0:2, :] = yrcv[t, 0, f, 2 * x : 2 * x + 2, :]
                W[t, f, x + 2, YH, ny - 2 : ny, :] = yrcv[t, 1, f, 2 * x : 2 * x + 2, :]
                at = f * rows + x
                W[t, f, x + 2, YZ, 0:1, :] = yzrcv[t, 0, at // ny, at % ny : at % ny + 1, :]
                W[t, f, x + 2, YZ, ny - 1 : ny, :] = yzrcv[t, 1, at // ny, at % ny : at % ny + 1, :]
            for k in range(2):
                at = k * rows + x
                W[t, 3 + k, x + 2, YH, 0:1, :] = yrcv[t, 0, 3, at : at + 1, :]
                W[t, 3 + k, x + 2, YH, ny - 1 : ny, :] = yrcv[t, 1, 3, at : at + 1, :]
        for n, (i, j) in enumerate(corners):
            xdst = rows + 2 if i < 0 else 1
            ydst = 0 if j < 0 else ny - 1
            for f in range(3):
                W[t, f, xdst, YH, ydst : ydst + 1, :] = crcv[t, n, f : f + 1, :]

        def field(x, q, fs=(0, 1, 2)):
            return [W[t, f, x, q] for f in fs]

        partner_y = {OWN: YH, YH: OWN, ZH: YZ}
        partner_z = {OWN: ZH, ZH: OWN, YH: YZ}

        def neighbours(x, q, fs=(0, 1, 2), with_x=True):
            c = field(x, q, fs)
            py = field(x, partner_y[q], fs)
            pz = field(x, partner_z[q], fs)
            n = len(fs)
            return c, [
                (field(x - 1, q, fs), field(x + 1, q, fs)),
                ([down_y(c[a], py[a]) for a in range(n)], [up_y(c[a], py[a]) for a in range(n)]),
                ([down_z(c[a], pz[a]) for a in range(n)], [up_z(c[a], pz[a]) for a in range(n)]),
            ]

        jx = {}
        partial = {}
        for x in range(1, rows + 3):
            inside = 2 <= x < rows + 2
            m = field(x, OWN, (3, 4))
            c, nb = neighbours(x, OWN)
            p, new, rate = phase_update(c, nb, m, theta[OWN])
            carried, slopes = carried_part(p, rate, nb)
            jx[x] = current(carried, slopes, 0)
            if inside:
                for a in range(3):
                    store(a, x - 2, new[a])
                phase_out[3, x - 2] = new[3]
                _, mb = neighbours(x, OWN, (3, 4))
                diff = [None, None]
                s = (c[0] + c[1]) + c[2]
                for d in range(3):
                    for side in range(2):
                        around = nb[d][side]
                        mob = 1.0 - 0.45 * (((around[0] + around[1]) + around[2]) + s)
                        for k in range(2):
                            flow = mob * (mb[d][side][k] - m[k])
                            diff[k] = flow if diff[k] is None else diff[k] + flow
                for k in range(2):
                    for a in range(4):
                        diff[k] = diff[k] - compositions[a][k] * rate[a]
                jy = current(carried, slopes, 1)
                jz = current(carried, slopes, 2)
                cb, nbb = neighbours(x, YH)
                pb, _, rb = phase_update(cb, nbb, field(x, YH, (3, 4)), theta[YH])
                jyb = current(*carried_part(pb, rb, nbb), 1)
                cz, nbz = neighbours(x, ZH)
                pz, _, rz = phase_update(cz, nbz, field(x, ZH, (3, 4)), theta[ZH])
                jzb = current(*carried_part(pz, rz, nbz), 2)
                for k in range(2):
                    dy = up_y(jy[k], jyb[k]) - down_y(jy[k], jyb[k])
                    above = jnp.where(upper & (lane == nl - 1), jz[k], up_z(jz[k], jzb[k]))
                    below = jnp.where(lower & (lane == 0), jz[k], down_z(jz[k], jzb[k]))
                    diff[k] = diff[k] - 0.5 * (dy + (above - below))
                partial[x] = (m, diff)
            if x >= 3:
                at = x - 1
                if 2 <= at < rows + 2:
                    m_at, diff_at = partial.pop(at)
                    for k in range(2):
                        total = diff_at[k] - 0.5 * (jx[at + 1][k] - jx[at - 1][k])
                        store(3 + k, at - 2, m_at[k] + time_step * total)
        for c in zcopies + copies:
            c.wait_send()

    def pair(tt, carry):
        def to_block(f, x, value):
            S[tt, f, x] = value

        def to_window(f, x, value):
            W[2 * tt + 2, f, x + 2, OWN] = value

        step(2 * tt, False, to_block)
        step(2 * tt + 1, True, to_window)
        return carry

    lax.fori_loop(0, STEPS // 2, pair, 0)
    for x in range(rows):
        for a in range(3):
            phase_out[a, x] = W[STEPS, a, x + 2, OWN]
        for k in range(2):
            pot_out[k, x] = W[STEPS, 3 + k, x + 2, OWN]


def on_device(labels, phase_noise, potentials, frame_shift):
    _, rows, ny, nl = phase_noise.shape
    vmem = pl.BlockSpec(memory_space=pltpu.VMEM)
    hbm = pl.BlockSpec(memory_space=pltpu.HBM)
    f32 = jnp.float32
    zrows = -(-3 * rows // ny)
    return pl.pallas_call(
        kernel,
        out_shape=(
            jax.ShapeDtypeStruct(phase_noise.shape, f32),
            jax.ShapeDtypeStruct(potentials.shape, f32),
        ),
        in_specs=[hbm] * 4,
        out_specs=(vmem, vmem),
        scratch_shapes=[
            pltpu.VMEM(labels.shape, jnp.int32),
            pltpu.VMEM(phase_noise.shape, f32),
            pltpu.VMEM(potentials.shape, f32),
            pltpu.SMEM(frame_shift.shape, jnp.int32),
            pltpu.SemaphoreType.DMA((4,)),
            pltpu.VMEM((STEPS // 2, 5, rows, ny, nl), f32),
            pltpu.VMEM((STEPS + 1, 5, rows + 4, 4, ny, nl), f32),
            pltpu.VMEM((STEPS, 2, 5, rows, ny, nl), f32),
            pltpu.VMEM((STEPS, 2, 4, ny, nl), f32),
            pltpu.VMEM((STEPS, 2, 4, ny, nl), f32),
            pltpu.VMEM((STEPS, 2, zrows, ny, nl), f32),
            pltpu.VMEM((STEPS, 2, zrows, ny, nl), f32),
            pltpu.VMEM((STEPS, 2, ny, nl), f32),
            pltpu.VMEM((STEPS, 2, ny, nl), f32),
            pltpu.VMEM((STEPS, 4, ny, nl), f32),
            pltpu.VMEM((STEPS, 4, ny, nl), f32),
            pltpu.SemaphoreType.DMA((STEPS, 16)),
            pltpu.SemaphoreType.DMA((STEPS, 16)),
        ],
        compiler_params=pltpu.CompilerParams(
            collective_id=0, has_side_effects=True, vmem_limit_bytes=16 * 1024 * 1024
        ),
        name="eutectic",
    )(labels, phase_noise, potentials, frame_shift)


def solution(mesh):
    placed = (P("gx", "gy"), P(None, "gx", "gy", "gz"), P(None, "gx", "gy", "gz"), P())
    return jax.shard_map(
        on_device,
        mesh=mesh,
        in_specs=placed,
        out_specs=(P(None, "gx", "gy", "gz"), P(None, "gx", "gy", "gz")),
        check_vma=False,
    )
```

```python
import functools
import math

import jax
import jax.numpy as jnp
from jax import lax
from jax.experimental import pallas as pl
from jax.experimental.pallas import tpu as pltpu
from jax.sharding import PartitionSpec as P

MESH = pl.DeviceIdType.MESH
STEPS = 4

interface_width = 4.0
time_step = 0.12
obstacle_coef = 16.0 / (math.pi * math.pi)
normal_floor = 0.25
surface_table = [
    [0.0, 1.0, 1.2, 0.9],
    [1.0, 0.0, 1.1, 1.0],
    [1.2, 1.1, 0.0, 0.8],
    [0.9, 1.0, 0.8, 0.0],
]
compositions = [[0.8, 0.1], [0.1, 0.8], [0.1, 0.1], [0.33, 0.33]]
latent_heat = [1.0, 0.9, 1.1, 0.0]
trapping_coef = math.pi * 4.0 / 4.0
undercool_span = 2.0

OWN, YH, ZH, YZ = 0, 1, 2, 3


def phase_update(center, nb, m, theta):
    lap = []
    for a in range(3):
        total = (nb[0][0][a] + nb[0][1][a]) + (nb[1][0][a] + nb[1][1][a])
        total = total + (nb[2][0][a] + nb[2][1][a])
        lap.append(total - 6.0 * center[a])
    lap.append(-(lap[0] + lap[1] + lap[2]))
    p = list(center) + [1.0 - (center[0] + center[1] + center[2])]

    def weigh(f, a):
        terms = [f[b] if surface_table[a][b] == 1.0 else surface_table[a][b] * f[b] for b in range(4) if b != a]
        return terms[0] + terms[1] + terms[2]

    drive = []
    for a in range(4):
        gp = weigh(p, a)
        gl = weigh(lap, a)
        v = gp * (obstacle_coef / interface_width - interface_width * lap[a]) + (interface_width * p[a]) * gl
        v = v - (compositions[a][0] * m[0] + compositions[a][1] * m[1])
        if latent_heat[a]:
            v = v + latent_heat[a] * theta
        drive.append(v)
    mean = 0.25 * ((drive[0] + drive[1]) + (drive[2] + drive[3]))
    q = [jnp.clip(p[a] - (time_step / interface_width) * (drive[a] - mean), 0.0, 1.0) for a in range(4)]
    inv = 1.0 / ((q[0] + q[1]) + (q[2] + q[3]))
    new = [q[a] * inv for a in range(4)]
    rate = [(new[a] - p[a]) * (1.0 / time_step) for a in range(4)]
    return p, new, rate


def carried_part(p, rate, nb):
    p3 = p[3] * 4.0
    carried, slopes = [], []
    for a in range(3):
        g = [0.5 * (nb[d][1][a] - nb[d][0][a]) for d in range(3)]
        square = g[0] * g[0] + g[1] * g[1] + g[2] * g[2]
        inv = lax.rsqrt(jnp.maximum(square, normal_floor * normal_floor))
        carried.append(p[a] * p3 * rate[a] * inv)
        slopes.append(g)
    return carried, slopes


def current(carried, slopes, d):
    out = []
    for k in range(2):
        total = None
        for a in range(3):
            term = (-trapping_coef * (compositions[3][k] - compositions[a][k])) * (carried[a] * slopes[a][d])
            total = term if total is None else total + term
        out.append(total)
    return out


def kernel(labels_hbm, noise_hbm, pot_hbm, shift_hbm, phase_out, pot_out,
           labels_ref, noise_ref, pot_ref, shift_ref, in_sem,
           S, W, zrcv, ysnd, yrcv, yzsnd, yzrcv, xzsnd, xzrcv, csnd, crcv, send_sem, recv_sem):
    fetches = [
        pltpu.make_async_copy(src, dst, in_sem.at[n])
        for n, (src, dst) in enumerate(
            ((labels_hbm, labels_ref), (noise_hbm, noise_ref), (pot_hbm, pot_ref), (shift_hbm, shift_ref))
        )
    ]
    for fetch in fetches:
        fetch.start()
    rows, ny, nl = noise_ref.shape[1:]
    gx, gy, gz = lax.axis_index("gx"), lax.axis_index("gy"), lax.axis_index("gz")
    nx_dev, ny_dev, nz_dev = lax.axis_size("gx"), lax.axis_size("gy"), lax.axis_size("gz")

    def near(index, count, step):
        return lax.rem(index + (count + step), count)

    xs = {-1: near(gx, nx_dev, -1), 1: near(gx, nx_dev, 1)}
    ys = {-1: near(gy, ny_dev, -1), 1: near(gy, ny_dev, 1)}
    zs = {-1: near(gz, nz_dev, -1), 1: near(gz, nz_dev, 1)}
    corners = [(-1, -1), (-1, 1), (1, -1), (1, 1)]
    targets = [{"gx": xs[i], "gy": ys[j]} for i, j in corners]
    targets += [{"gx": xs[-1]}, {"gx": xs[1]}, {"gy": ys[-1]}, {"gy": ys[1]}, {"gz": zs[-1]}, {"gz": zs[1]}]

    barrier = pltpu.get_barrier_semaphore()
    for target in targets:
        pl.semaphore_signal(barrier, inc=1, device_id=target, device_id_type=MESH)

    lane = lax.broadcasted_iota(jnp.int32, (ny, nl), 1)
    row = lax.broadcasted_iota(jnp.int32, (ny, nl), 0)
    lower = gz == 0
    upper = gz == nz_dev - 1
    total_planes = nl * nz_dev
    front = total_planes // 2
    zown = gz * nl + lane
    zhalo = jnp.where(lane < nl // 2, zown + nl, zown - nl)

    def theta_of(index):
        return undercool_span * (index.astype(jnp.float32) + 0.5 - front) / total_planes

    theta = {OWN: theta_of(zown), ZH: theta_of(zhalo)}
    theta[YH] = theta[OWN]
    solid = zown < front

    def up_y(a, b):
        return pltpu.roll(jnp.where(row == 0, b, a), ny - 1, 0)

    def down_y(a, b):
        return pltpu.roll(jnp.where(row == ny - 1, b, a), 1, 0)

    def up_z(a, b):
        return pltpu.roll(jnp.where(lane == 0, b, a), nl - 1, 1)

    def down_z(a, b):
        return pltpu.roll(jnp.where(lane == nl - 1, b, a), 1, 1)

    for fetch in fetches:
        fetch.wait()
    first_shift, second_shift = shift_ref[0], shift_ref[1]
    lrow = lax.broadcasted_iota(jnp.int32, (ny, ny), 0)
    lcol = lax.broadcasted_iota(jnp.int32, (ny, ny), 1)
    for x in range(rows):
        lab = jnp.broadcast_to(labels_ref[x : x + 1, :].astype(jnp.float32), (ny, ny))
        lab = jnp.sum(jnp.where(lrow == lcol, lab, 0.0), axis=1, keepdims=True)
        lab = jnp.broadcast_to(lab, (ny, nl))
        init = []
        for a in range(3):
            init.append(noise_ref[a, x] + jnp.where((lab == float(a)) & solid, 1.0, 0.0))
        init.append(noise_ref[3, x] + jnp.where(solid, 0.0, 1.0))
        inv = 1.0 / ((init[0] + init[1]) + (init[2] + init[3]))
        for a in range(3):
            W[0, a, x + 2, OWN] = init[a] * inv
        for k in range(2):
            W[0, 3 + k, x + 2, OWN] = pot_ref[k, x]

    pl.semaphore_wait(barrier, len(targets))

    def step(t, shifted, store):
        def copy(src, dst, n, target):
            return pltpu.make_async_remote_copy(
                src_ref=src, dst_ref=dst, send_sem=send_sem.at[t, n], recv_sem=recv_sem.at[t, n],
                device_id=target, device_id_type=MESH,
            )

        block = S.at[t // 2] if shifted else W.at[t, pl.ds(0, 5), pl.ds(2, rows), OWN]
        zcopies = [
            copy(block, zrcv.at[t, 0], 0, {"gz": zs[1]}),
            copy(block, zrcv.at[t, 1], 1, {"gz": zs[-1]}),
        ]
        for c in zcopies:
            c.start()

        copies = []

        def launch(c):
            c.start()
            copies.append(c)

        def pack_own(x, f, own):
            if f < 3:
                ysnd[t, 0, f, 2 * x : 2 * x + 2, :] = own[0:2]
                ysnd[t, 1, f, 2 * x : 2 * x + 2, :] = own[ny - 2 : ny]
                for n, (i, j) in enumerate(corners):
                    if x == (0 if i < 0 else rows - 1):
                        csnd[t, n, f : f + 1, :] = own[0:1] if j < 0 else own[ny - 1 : ny]
            else:
                at = (f - 3) * rows + x
                ysnd[t, 0, 3, at : at + 1, :] = own[0:1]
                ysnd[t, 1, 3, at : at + 1, :] = own[ny - 1 : ny]

        def send_own():
            low, high = (2, rows + 2), (rows, 0)
            for side, (src, dst) in ((-1, low), (1, high)):
                base = 6 + (0 if side < 0 else 2)
                edge_src = 2 if side < 0 else rows + 1
                edge_dst = rows + 2 if side < 0 else 1
                target = {"gx": xs[side]}
                launch(copy(W.at[t, pl.ds(0, 3), pl.ds(src, 2), OWN], W.at[t, pl.ds(0, 3), pl.ds(dst, 2), OWN], base, target))
                launch(copy(W.at[t, pl.ds(3, 2), edge_src, OWN], W.at[t, pl.ds(3, 2), edge_dst, OWN], base + 1, target))

        def send_y():
            for n, (i, j) in enumerate(corners):
                launch(copy(csnd.at[t, n], crcv.at[t, n], 2 + n, {"gx": xs[i], "gy": ys[j]}))
            launch(copy(ysnd.at[t, 0], yrcv.at[t, 0], 10, {"gy": ys[-1]}))
            launch(copy(ysnd.at[t, 1], yrcv.at[t, 1], 11, {"gy": ys[1]}))

        if not shifted:
            for x in range(rows):
                for f in range(5):
                    pack_own(x, f, W[t, f, x + 2, OWN])
            send_y()
            send_own()
        for c in zcopies:
            c.wait_recv()
        if shifted:
            shift = jnp.full((ny, nl), jnp.where(t == 1, first_shift, second_shift), jnp.int32)
            bits = [(shift & 1) != 0, (shift & 2) != 0, (shift & 4) != 0, (shift & 8) != 0]
        packed = {}
        for x in range(rows):
            for f in range(5):
                own = S[t // 2, f, x] if shifted else W[t, f, x + 2, OWN]
                halo = jnp.where(lane < nl // 2, zrcv[t, 1, f, x], zrcv[t, 0, f, x])
                if shifted:
                    halo = jnp.where(upper & (lane < nl // 2), 0.0, halo)
                    for bit in range(4):
                        by = 1 << bit
                        mixed_own = jnp.where(lane < by, halo, own)
                        mixed_halo = jnp.where(lane < by, own, halo)
                        own = jnp.where(bits[bit], pltpu.roll(mixed_own, nl - by, 1), own)
                        halo = jnp.where(bits[bit], pltpu.roll(mixed_halo, nl - by, 1), halo)
                    W[t, f, x + 2, OWN] = own
                    pack_own(x, f, own)
                first = jnp.broadcast_to(own[:, 0:1], (ny, nl))
                last = jnp.broadcast_to(own[:, nl - 1 : nl], (ny, nl))
                halo = jnp.where(upper & (lane < nl // 2), last, halo)
                halo = jnp.where(lower & (lane >= nl // 2), first, halo)
                W[t, f, x + 2, ZH] = halo
                if f < 3:
                    at = f * rows + x
                    yzsnd[t, 0, at // ny, at % ny : at % ny + 1, :] = halo[0:1]
                    yzsnd[t, 1, at // ny, at % ny : at % ny + 1, :] = halo[ny - 1 : ny]
                    if x == 0 or x == rows - 1:
                        mixed = halo if f == 0 else jnp.where(
                            (lane == 8 * f) | (lane == 8 * f - 1), pltpu.roll(halo, 8 * f, 1), packed[x])
                        packed[x] = mixed
        xzsnd[t, 0] = packed[0]
        xzsnd[t, 1] = packed[rows - 1]
        if shifted:
            send_y()
        launch(copy(xzsnd.at[t, 0], xzrcv.at[t, 0], 12, {"gx": xs[-1]}))
        launch(copy(xzsnd.at[t, 1], xzrcv.at[t, 1], 13, {"gx": xs[1]}))
        launch(copy(yzsnd.at[t, 0], yzrcv.at[t, 0], 14, {"gy": ys[-1]}))
        launch(copy(yzsnd.at[t, 1], yzrcv.at[t, 1], 15, {"gy": ys[1]}))
        if shifted:
            send_own()
        for c in copies:
            c.wait_recv()

        for f in range(3):
            by = 8 * f
            for slot, xdst in ((0, rows + 2), (1, 1)):
                halo = xzrcv[t, slot]
                W[t, f, xdst, ZH] = pltpu.roll(halo, nl - by, 1) if by else halo
        for x in range(rows):
            for f in range(3):
                W[t, f, x + 2, YH, 0:2, :] = yrcv[t, 0, f, 2 * x : 2 * x + 2, :]
                W[t, f, x + 2, YH, ny - 2 : ny, :] = yrcv[t, 1, f, 2 * x : 2 * x + 2, :]
                at = f * rows + x
                W[t, f, x + 2, YZ, 0:1, :] = yzrcv[t, 0, at // ny, at % ny : at % ny + 1, :]
                W[t, f, x + 2, YZ, ny - 1 : ny, :] = yzrcv[t, 1, at // ny, at % ny : at % ny + 1, :]
            for k in range(2):
                at = k * rows + x
                W[t, 3 + k, x + 2, YH, 0:1, :] = yrcv[t, 0, 3, at : at + 1, :]
                W[t, 3 + k, x + 2, YH, ny - 1 : ny, :] = yrcv[t, 1, 3, at : at + 1, :]
        for n, (i, j) in enumerate(corners):
            xdst = rows + 2 if i < 0 else 1
            ydst = 0 if j < 0 else ny - 1
            for f in range(3):
                W[t, f, xdst, YH, ydst : ydst + 1, :] = crcv[t, n, f : f + 1, :]

        def field(x, q, fs=(0, 1, 2)):
            return [W[t, f, x, q] for f in fs]

        partner_y = {OWN: YH, YH: OWN, ZH: YZ}
        partner_z = {OWN: ZH, ZH: OWN, YH: YZ}

        def neighbours(x, q, fs=(0, 1, 2), with_x=True):
            c = field(x, q, fs)
            py = field(x, partner_y[q], fs)
            pz = field(x, partner_z[q], fs)
            n = len(fs)
            return c, [
                (field(x - 1, q, fs), field(x + 1, q, fs)),
                ([down_y(c[a], py[a]) for a in range(n)], [up_y(c[a], py[a]) for a in range(n)]),
                ([down_z(c[a], pz[a]) for a in range(n)], [up_z(c[a], pz[a]) for a in range(n)]),
            ]

        jx = {}
        partial = {}
        for x in range(1, rows + 3):
            inside = 2 <= x < rows + 2
            m = field(x, OWN, (3, 4))
            c, nb = neighbours(x, OWN)
            p, new, rate = phase_update(c, nb, m, theta[OWN])
            carried, slopes = carried_part(p, rate, nb)
            jx[x] = current(carried, slopes, 0)
            if inside:
                for a in range(3):
                    store(a, x - 2, new[a])
                phase_out[3, x - 2] = new[3]
                _, mb = neighbours(x, OWN, (3, 4))
                diff = [None, None]
                s = (c[0] + c[1]) + c[2]
                for d in range(3):
                    for side in range(2):
                        around = nb[d][side]
                        mob = 1.0 - 0.45 * (((around[0] + around[1]) + around[2]) + s)
                        for k in range(2):
                            flow = mob * (mb[d][side][k] - m[k])
                            diff[k] = flow if diff[k] is None else diff[k] + flow
                for k in range(2):
                    for a in range(4):
                        diff[k] = diff[k] - compositions[a][k] * rate[a]
                jy = current(carried, slopes, 1)
                jz = current(carried, slopes, 2)
                cb, nbb = neighbours(x, YH)
                pb, _, rb = phase_update(cb, nbb, field(x, YH, (3, 4)), theta[YH])
                jyb = current(*carried_part(pb, rb, nbb), 1)
                cz, nbz = neighbours(x, ZH)
                pz, _, rz = phase_update(cz, nbz, field(x, ZH, (3, 4)), theta[ZH])
                jzb = current(*carried_part(pz, rz, nbz), 2)
                for k in range(2):
                    dy = up_y(jy[k], jyb[k]) - down_y(jy[k], jyb[k])
                    above = jnp.where(upper & (lane == nl - 1), jz[k], up_z(jz[k], jzb[k]))
                    below = jnp.where(lower & (lane == 0), jz[k], down_z(jz[k], jzb[k]))
                    diff[k] = diff[k] - 0.5 * (dy + (above - below))
                partial[x] = (m, diff)
            if x >= 3:
                at = x - 1
                if 2 <= at < rows + 2:
                    m_at, diff_at = partial.pop(at)
                    for k in range(2):
                        total = diff_at[k] - 0.5 * (jx[at + 1][k] - jx[at - 1][k])
                        store(3 + k, at - 2, m_at[k] + time_step * total)
        for c in zcopies + copies:
            c.wait_send()

    def pair(tt, carry):
        def to_block(f, x, value):
            S[tt, f, x] = value

        def to_window(f, x, value):
            W[2 * tt + 2, f, x + 2, OWN] = value

        step(2 * tt, False, to_block)
        step(2 * tt + 1, True, to_window)
        return carry

    lax.fori_loop(0, STEPS // 2, pair, 0)
    for x in range(rows):
        for a in range(3):
            phase_out[a, x] = W[STEPS, a, x + 2, OWN]
        for k in range(2):
            pot_out[k, x] = W[STEPS, 3 + k, x + 2, OWN]


def on_device(labels, phase_noise, potentials, frame_shift):
    _, rows, ny, nl = phase_noise.shape
    vmem = pl.BlockSpec(memory_space=pltpu.VMEM)
    hbm = pl.BlockSpec(memory_space=pltpu.HBM)
    f32 = jnp.float32
    zrows = -(-3 * rows // ny)
    return pl.pallas_call(
        kernel,
        out_shape=(pltpu.VMEM(phase_noise.shape, f32), pltpu.VMEM(potentials.shape, f32)),
        in_specs=[hbm] * 4,
        out_specs=(vmem, vmem),
        scratch_shapes=[
            pltpu.VMEM(labels.shape, jnp.int32),
            pltpu.VMEM(phase_noise.shape, f32),
            pltpu.VMEM(potentials.shape, f32),
            pltpu.SMEM(frame_shift.shape, jnp.int32),
            pltpu.SemaphoreType.DMA((4,)),
            pltpu.VMEM((STEPS // 2, 5, rows, ny, nl), f32),
            pltpu.VMEM((STEPS + 1, 5, rows + 4, 4, ny, nl), f32),
            pltpu.VMEM((STEPS, 2, 5, rows, ny, nl), f32),
            pltpu.VMEM((STEPS, 2, 4, ny, nl), f32),
            pltpu.VMEM((STEPS, 2, 4, ny, nl), f32),
            pltpu.VMEM((STEPS, 2, zrows, ny, nl), f32),
            pltpu.VMEM((STEPS, 2, zrows, ny, nl), f32),
            pltpu.VMEM((STEPS, 2, ny, nl), f32),
            pltpu.VMEM((STEPS, 2, ny, nl), f32),
            pltpu.VMEM((STEPS, 4, ny, nl), f32),
            pltpu.VMEM((STEPS, 4, ny, nl), f32),
            pltpu.SemaphoreType.DMA((STEPS, 16)),
            pltpu.SemaphoreType.DMA((STEPS, 16)),
        ],
        compiler_params=pltpu.CompilerParams(collective_id=0, has_side_effects=True),
        name="eutectic",
    )(labels, phase_noise, potentials, frame_shift)


def solution(mesh):
    placed = (P("gx", "gy"), P(None, "gx", "gy", "gz"), P(None, "gx", "gy", "gz"), P())
    return jax.shard_map(
        on_device,
        mesh=mesh,
        in_specs=placed,
        out_specs=(P(None, "gx", "gy", "gz"), P(None, "gx", "gy", "gz")),
        check_vma=False,
    )
```

```python
import functools
import math

import jax
import jax.numpy as jnp
from jax import lax
from jax.experimental import pallas as pl
from jax.experimental.pallas import tpu as pltpu
from jax.sharding import PartitionSpec as P

MESH = pl.DeviceIdType.MESH
STEPS = 4

interface_width = 4.0
time_step = 0.12
obstacle_coef = 16.0 / (math.pi * math.pi)
normal_floor = 0.25
surface_table = [
    [0.0, 1.0, 1.2, 0.9],
    [1.0, 0.0, 1.1, 1.0],
    [1.2, 1.1, 0.0, 0.8],
    [0.9, 1.0, 0.8, 0.0],
]
compositions = [[0.8, 0.1], [0.1, 0.8], [0.1, 0.1], [0.33, 0.33]]
latent_heat = [1.0, 0.9, 1.1, 0.0]
trapping_coef = math.pi * 4.0 / 4.0
undercool_span = 2.0

OWN, YH, ZH, YZ = 0, 1, 2, 3


def phase_update(center, nb, m, theta):
    lap = []
    for a in range(3):
        total = (nb[0][0][a] + nb[0][1][a]) + (nb[1][0][a] + nb[1][1][a])
        total = total + (nb[2][0][a] + nb[2][1][a])
        lap.append(total - 6.0 * center[a])
    lap.append(-(lap[0] + lap[1] + lap[2]))
    p = list(center) + [1.0 - (center[0] + center[1] + center[2])]

    def weigh(f, a):
        terms = [f[b] if surface_table[a][b] == 1.0 else surface_table[a][b] * f[b] for b in range(4) if b != a]
        return terms[0] + terms[1] + terms[2]

    drive = []
    for a in range(4):
        gp = weigh(p, a)
        gl = weigh(lap, a)
        v = gp * (obstacle_coef / interface_width - interface_width * lap[a]) + (interface_width * p[a]) * gl
        v = v - (compositions[a][0] * m[0] + compositions[a][1] * m[1])
        if latent_heat[a]:
            v = v + latent_heat[a] * theta
        drive.append(v)
    mean = 0.25 * ((drive[0] + drive[1]) + (drive[2] + drive[3]))
    q = [jnp.clip(p[a] - (time_step / interface_width) * (drive[a] - mean), 0.0, 1.0) for a in range(4)]
    inv = 1.0 / ((q[0] + q[1]) + (q[2] + q[3]))
    new = [q[a] * inv for a in range(4)]
    rate = [(new[a] - p[a]) * (1.0 / time_step) for a in range(4)]
    return p, new, rate


def carried_part(p, rate, nb):
    p3 = p[3] * 4.0
    carried, slopes = [], []
    for a in range(3):
        g = [0.5 * (nb[d][1][a] - nb[d][0][a]) for d in range(3)]
        square = g[0] * g[0] + g[1] * g[1] + g[2] * g[2]
        inv = lax.rsqrt(jnp.maximum(square, normal_floor * normal_floor))
        carried.append(p[a] * p3 * rate[a] * inv)
        slopes.append(g)
    return carried, slopes


def current(carried, slopes, d):
    out = []
    for k in range(2):
        total = None
        for a in range(3):
            term = (-trapping_coef * (compositions[3][k] - compositions[a][k])) * (carried[a] * slopes[a][d])
            total = term if total is None else total + term
        out.append(total)
    return out


def kernel(labels_hbm, noise_hbm, pot_hbm, shift_hbm, phase_out, pot_out,
           labels_ref, noise_ref, pot_ref, shift_ref, in_sem,
           S, W, zrcv, ysnd, yrcv, yzsnd, yzrcv, xzsnd, xzrcv, csnd, crcv, czsnd, czrcv, send_sem, recv_sem):
    fetches = [
        pltpu.make_async_copy(src, dst, in_sem.at[n])
        for n, (src, dst) in enumerate(
            ((labels_hbm, labels_ref), (noise_hbm, noise_ref), (pot_hbm, pot_ref), (shift_hbm, shift_ref))
        )
    ]
    for fetch in fetches:
        fetch.start()
    rows, ny, nl = noise_ref.shape[1:]
    gx, gy, gz = lax.axis_index("gx"), lax.axis_index("gy"), lax.axis_index("gz")
    nx_dev, ny_dev, nz_dev = lax.axis_size("gx"), lax.axis_size("gy"), lax.axis_size("gz")

    def near(index, count, step):
        return lax.rem(index + (count + step), count)

    xs = {-1: near(gx, nx_dev, -1), 1: near(gx, nx_dev, 1)}
    ys = {-1: near(gy, ny_dev, -1), 1: near(gy, ny_dev, 1)}
    zs = {-1: near(gz, nz_dev, -1), 1: near(gz, nz_dev, 1)}
    corners = [(-1, -1), (-1, 1), (1, -1), (1, 1)]
    targets = [{"gx": xs[i], "gy": ys[j]} for i, j in corners]
    targets += [{"gx": xs[-1]}, {"gx": xs[1]}, {"gy": ys[-1]}, {"gy": ys[1]}, {"gz": zs[-1]}, {"gz": zs[1]}]

    barrier = pltpu.get_barrier_semaphore()
    for target in targets:
        pl.semaphore_signal(barrier, inc=1, device_id=target, device_id_type=MESH)

    lane = lax.broadcasted_iota(jnp.int32, (ny, nl), 1)
    row = lax.broadcasted_iota(jnp.int32, (ny, nl), 0)
    lower = gz == 0
    upper = gz == nz_dev - 1
    total_planes = nl * nz_dev
    front = total_planes // 2
    zown = gz * nl + lane
    zhalo = jnp.where(lane < nl // 2, zown + nl, zown - nl)

    def theta_of(index):
        return undercool_span * (index.astype(jnp.float32) + 0.5 - front) / total_planes

    theta = {OWN: theta_of(zown), ZH: theta_of(zhalo)}
    theta[YH] = theta[OWN]
    solid = zown < front

    def up_y(a, b):
        return pltpu.roll(jnp.where(row == 0, b, a), ny - 1, 0)

    def down_y(a, b):
        return pltpu.roll(jnp.where(row == ny - 1, b, a), 1, 0)

    def up_z(a, b):
        return pltpu.roll(jnp.where(lane == 0, b, a), nl - 1, 1)

    def down_z(a, b):
        return pltpu.roll(jnp.where(lane == nl - 1, b, a), 1, 1)

    for fetch in fetches:
        fetch.wait()
    first_shift, second_shift = shift_ref[0], shift_ref[1]
    lrow = lax.broadcasted_iota(jnp.int32, (ny, ny), 0)
    lcol = lax.broadcasted_iota(jnp.int32, (ny, ny), 1)
    for x in range(rows):
        lab = jnp.broadcast_to(labels_ref[x : x + 1, :].astype(jnp.float32), (ny, ny))
        lab = jnp.sum(jnp.where(lrow == lcol, lab, 0.0), axis=1, keepdims=True)
        lab = jnp.broadcast_to(lab, (ny, nl))
        init = []
        for a in range(3):
            init.append(noise_ref[a, x] + jnp.where((lab == float(a)) & solid, 1.0, 0.0))
        init.append(noise_ref[3, x] + jnp.where(solid, 0.0, 1.0))
        inv = 1.0 / ((init[0] + init[1]) + (init[2] + init[3]))
        for a in range(3):
            W[0, a, x + 2, OWN] = init[a] * inv
        for k in range(2):
            W[0, 3 + k, x + 2, OWN] = pot_ref[k, x]

    pl.semaphore_wait(barrier, len(targets))

    def step(t, shifted, store):
        def copy(src, dst, n, target):
            return pltpu.make_async_remote_copy(
                src_ref=src, dst_ref=dst, send_sem=send_sem.at[t, n], recv_sem=recv_sem.at[t, n],
                device_id=target, device_id_type=MESH,
            )

        block = S.at[t // 2] if shifted else W.at[t, pl.ds(0, 5), pl.ds(2, rows), OWN]
        zcopies = [
            copy(block, zrcv.at[t, 0], 0, {"gz": zs[1]}),
            copy(block, zrcv.at[t, 1], 1, {"gz": zs[-1]}),
        ]
        for c in zcopies:
            c.start()

        copies = []

        def launch(c):
            c.start()
            copies.append(c)

        def pack_own(x, f, own):
            if f < 3:
                ysnd[t, 0, f, 2 * x : 2 * x + 2, :] = own[0:2]
                ysnd[t, 1, f, 2 * x : 2 * x + 2, :] = own[ny - 2 : ny]
                for n, (i, j) in enumerate(corners):
                    if x == (0 if i < 0 else rows - 1):
                        csnd[t, n, f : f + 1, :] = own[0:1] if j < 0 else own[ny - 1 : ny]
            else:
                at = (f - 3) * rows + x
                ysnd[t, 0, 3, at : at + 1, :] = own[0:1]
                ysnd[t, 1, 3, at : at + 1, :] = own[ny - 1 : ny]

        def send_own():
            low, high = (2, rows + 2), (rows, 0)
            for side, (src, dst) in ((-1, low), (1, high)):
                base = 6 + (0 if side < 0 else 2)
                edge_src = 2 if side < 0 else rows + 1
                edge_dst = rows + 2 if side < 0 else 1
                target = {"gx": xs[side]}
                faces = S.at[t // 2, pl.ds(0, 3), pl.ds(src - 2, 2)] if shifted else W.at[t, pl.ds(0, 3), pl.ds(src, 2), OWN]
                chem = S.at[t // 2, pl.ds(3, 2), edge_src - 2] if shifted else W.at[t, pl.ds(3, 2), edge_src, OWN]
                launch(copy(faces, W.at[t, pl.ds(0, 3), pl.ds(dst, 2), OWN], base, target))
                launch(copy(chem, W.at[t, pl.ds(3, 2), edge_dst, OWN], base + 1, target))

        def send_y():
            for n, (i, j) in enumerate(corners):
                launch(copy(csnd.at[t, n], crcv.at[t, n], 2 + n, {"gx": xs[i], "gy": ys[j]}))
            launch(copy(ysnd.at[t, 0], yrcv.at[t, 0], 10, {"gy": ys[-1]}))
            launch(copy(ysnd.at[t, 1], yrcv.at[t, 1], 11, {"gy": ys[1]}))

        def source(x, f):
            return S[t // 2, f, x] if shifted else W[t, f, x + 2, OWN]

        for x in range(rows):
            for f in range(5):
                pack_own(x, f, source(x, f))
        send_y()
        send_own()
        for c in zcopies:
            c.wait_recv()

        def clamp(own, halo):
            first = jnp.broadcast_to(own[:, 0:1], (ny, nl))
            last = jnp.broadcast_to(own[:, nl - 1 : nl], (ny, nl))
            halo = jnp.where(upper & (lane < nl // 2), last, halo)
            return jnp.where(lower & (lane >= nl // 2), first, halo)

        if shifted:
            shift = jnp.full((ny, nl), jnp.where(t == 1, first_shift, second_shift), jnp.int32)
            bits = [(shift & 1) != 0, (shift & 2) != 0, (shift & 4) != 0, (shift & 8) != 0]

        def moved(own, halo):
            for bit in range(4):
                by = 1 << bit
                mixed_own = jnp.where(lane < by, halo, own)
                mixed_halo = jnp.where(lane < by, own, halo)
                own = jnp.where(bits[bit], pltpu.roll(mixed_own, nl - by, 1), own)
                halo = jnp.where(bits[bit], pltpu.roll(mixed_halo, nl - by, 1), halo)
            return own, halo

        def roll_by(value, by):
            return pltpu.roll(value, by % nl, 1) if by % nl else value

        packed = [None, None]

        def pack_edge(side, at, width, low, value):
            inside = (lane >= width * at - low) & (lane < width * (at + 1) - low)
            if at == 0:
                packed[side] = value
            else:
                packed[side] = jnp.where(inside, roll_by(value, width * at), packed[side])

        for f in range(5):
            for x in range(rows):
                if shifted:
                    above = jnp.where(upper, 0.0, zrcv[t, 1, f, x])
                    if f < 3:
                        yzsnd[t, 0, f, 2 * x : 2 * x + 2, :] = above[0:2]
                        yzsnd[t, 1, f, 2 * x : 2 * x + 2, :] = above[ny - 2 : ny]
                        for n, (i, j) in enumerate(corners):
                            if x == (0 if i < 0 else rows - 1):
                                czsnd[t, n, f : f + 1, :] = above[0:1] if j < 0 else above[ny - 1 : ny]
                        if x < 2:
                            pack_edge(0, 2 * f + x, 16, 0, above)
                        if x >= rows - 2 and (f or x == rows - 1):
                            pack_edge(1, 2 * f + (rows - 1 - x), 16, 0, above)
                    else:
                        at = (f - 3) * rows + x
                        yzsnd[t, 0, 3, at : at + 1, :] = above[0:1]
                        yzsnd[t, 1, 3, at : at + 1, :] = above[ny - 1 : ny]
                        if x == 0:
                            pack_edge(0, 6 + f - 3, 16, 0, above)
                        if x == rows - 1:
                            pack_edge(1, 6 + f - 3, 16, 0, above)
                    if f == 0 and x == rows - 1:
                        second = jnp.where(upper, 0.0, zrcv[t, 1, 0, rows - 2])
                        pack_edge(1, 1, 16, 0, second)
                else:
                    own = source(x, f)
                    halo = clamp(own, jnp.where(lane < nl // 2, zrcv[t, 1, f, x], zrcv[t, 0, f, x]))
                    W[t, f, x + 2, ZH] = halo
                    if f < 3:
                        yzsnd[t, 0, f, 2 * x : 2 * x + 1, :] = halo[0:1]
                        yzsnd[t, 1, f, 2 * x + 1 : 2 * x + 2, :] = halo[ny - 1 : ny]
                        if x == 0:
                            pack_edge(0, f, 8, 1, halo)
                        if x == rows - 1:
                            pack_edge(1, f, 8, 1, halo)
        xzsnd[t, 0] = packed[0]
        xzsnd[t, 1] = packed[1]
        if shifted:
            for n, (i, j) in enumerate(corners):
                launch(copy(czsnd.at[t, n], czrcv.at[t, n], 16 + n, {"gx": xs[i], "gy": ys[j]}))
        launch(copy(yzsnd.at[t, 0], yzrcv.at[t, 0], 14, {"gy": ys[-1]}))
        launch(copy(yzsnd.at[t, 1], yzrcv.at[t, 1], 15, {"gy": ys[1]}))
        launch(copy(xzsnd.at[t, 0], xzrcv.at[t, 0], 12, {"gx": xs[-1]}))
        launch(copy(xzsnd.at[t, 1], xzrcv.at[t, 1], 13, {"gx": xs[1]}))
        if shifted:
            for x in range(rows):
                for f in range(5):
                    above = jnp.where(upper, 0.0, zrcv[t, 1, f, x])
                    halo = jnp.where(lane < nl // 2, above, zrcv[t, 0, f, x])
                    own, halo = moved(source(x, f), halo)
                    W[t, f, x + 2, OWN] = own
                    W[t, f, x + 2, ZH] = clamp(own, halo)
        for c in copies:
            c.wait_recv()

        for slot, edge, outer in ((0, rows + 2, rows + 3), (1, 1, 0)):
            halo_pack = xzrcv[t, slot]
            for f in range(5):
                if not shifted:
                    if f < 3:
                        W[t, f, edge, ZH] = roll_by(halo_pack, nl - 8 * f)
                    continue
                at = 2 * f if f < 3 else 6 + f - 3
                own, halo = moved(W[t, f, edge, OWN], roll_by(halo_pack, nl - 16 * at))
                W[t, f, edge, OWN] = own
                if f < 3:
                    W[t, f, edge, ZH] = clamp(own, halo)
                    W[t, f, outer, OWN] = moved(W[t, f, outer, OWN], roll_by(halo_pack, nl - 16 * (at + 1)))[0]

        for f in range(4):
            faces = []
            for slot in range(2):
                own, halo = yrcv[t, slot, f], yzrcv[t, slot, f]
                if shifted:
                    own, halo = moved(own, halo)
                    if f < 3:
                        halo = clamp(own, halo)
                faces.append((own, halo))
            for x in range(rows):
                if f < 3:
                    W[t, f, x + 2, YH, 0:2, :] = faces[0][0][2 * x : 2 * x + 2]
                    W[t, f, x + 2, YH, ny - 2 : ny, :] = faces[1][0][2 * x : 2 * x + 2]
                    W[t, f, x + 2, YZ, 0:1, :] = faces[0][1][2 * x : 2 * x + 1]
                    W[t, f, x + 2, YZ, ny - 1 : ny, :] = faces[1][1][2 * x + 1 : 2 * x + 2]
                else:
                    for k in range(2):
                        at = k * rows + x
                        W[t, 3 + k, x + 2, YH, 0:1, :] = faces[0][0][at : at + 1]
                        W[t, 3 + k, x + 2, YH, ny - 1 : ny, :] = faces[1][0][at : at + 1]
        for n, (i, j) in enumerate(corners):
            xdst = rows + 2 if i < 0 else 1
            ydst = 0 if j < 0 else ny - 1
            own = crcv[t, n]
            if shifted:
                own, _ = moved(own, czrcv[t, n])
            for f in range(3):
                W[t, f, xdst, YH, ydst : ydst + 1, :] = own[f : f + 1]

        def field(x, q, fs=(0, 1, 2)):
            return [W[t, f, x, q] for f in fs]

        partner_y = {OWN: YH, YH: OWN, ZH: YZ}
        partner_z = {OWN: ZH, ZH: OWN, YH: YZ}

        def neighbours(x, q, fs=(0, 1, 2), with_x=True):
            c = field(x, q, fs)
            py = field(x, partner_y[q], fs)
            pz = field(x, partner_z[q], fs)
            n = len(fs)
            return c, [
                (field(x - 1, q, fs), field(x + 1, q, fs)),
                ([down_y(c[a], py[a]) for a in range(n)], [up_y(c[a], py[a]) for a in range(n)]),
                ([down_z(c[a], pz[a]) for a in range(n)], [up_z(c[a], pz[a]) for a in range(n)]),
            ]

        jx = {}
        partial = {}
        for x in range(1, rows + 3):
            inside = 2 <= x < rows + 2
            m = field(x, OWN, (3, 4))
            c, nb = neighbours(x, OWN)
            p, new, rate = phase_update(c, nb, m, theta[OWN])
            carried, slopes = carried_part(p, rate, nb)
            jx[x] = current(carried, slopes, 0)
            if inside:
                for a in range(3):
                    store(a, x - 2, new[a])
                phase_out[3, x - 2] = new[3]
                _, mb = neighbours(x, OWN, (3, 4))
                diff = [None, None]
                s = (c[0] + c[1]) + c[2]
                for d in range(3):
                    for side in range(2):
                        around = nb[d][side]
                        mob = 1.0 - 0.45 * (((around[0] + around[1]) + around[2]) + s)
                        for k in range(2):
                            flow = mob * (mb[d][side][k] - m[k])
                            diff[k] = flow if diff[k] is None else diff[k] + flow
                for k in range(2):
                    for a in range(4):
                        diff[k] = diff[k] - compositions[a][k] * rate[a]
                jy = current(carried, slopes, 1)
                jz = current(carried, slopes, 2)
                cb, nbb = neighbours(x, YH)
                pb, _, rb = phase_update(cb, nbb, field(x, YH, (3, 4)), theta[YH])
                jyb = current(*carried_part(pb, rb, nbb), 1)
                cz, nbz = neighbours(x, ZH)
                pz, _, rz = phase_update(cz, nbz, field(x, ZH, (3, 4)), theta[ZH])
                jzb = current(*carried_part(pz, rz, nbz), 2)
                for k in range(2):
                    dy = up_y(jy[k], jyb[k]) - down_y(jy[k], jyb[k])
                    above = jnp.where(upper & (lane == nl - 1), jz[k], up_z(jz[k], jzb[k]))
                    below = jnp.where(lower & (lane == 0), jz[k], down_z(jz[k], jzb[k]))
                    diff[k] = diff[k] - 0.5 * (dy + (above - below))
                partial[x] = (m, diff)
            if x >= 3:
                at = x - 1
                if 2 <= at < rows + 2:
                    m_at, diff_at = partial.pop(at)
                    for k in range(2):
                        total = diff_at[k] - 0.5 * (jx[at + 1][k] - jx[at - 1][k])
                        store(3 + k, at - 2, m_at[k] + time_step * total)
        for c in zcopies + copies:
            c.wait_send()

    def pair(tt, carry):
        def to_block(f, x, value):
            S[tt, f, x] = value

        def to_window(f, x, value):
            W[2 * tt + 2, f, x + 2, OWN] = value

        step(2 * tt, False, to_block)
        step(2 * tt + 1, True, to_window)
        return carry

    lax.fori_loop(0, STEPS // 2, pair, 0)
    for x in range(rows):
        for a in range(3):
            phase_out[a, x] = W[STEPS, a, x + 2, OWN]
        for k in range(2):
            pot_out[k, x] = W[STEPS, 3 + k, x + 2, OWN]


def on_device(labels, phase_noise, potentials, frame_shift):
    _, rows, ny, nl = phase_noise.shape
    vmem = pl.BlockSpec(memory_space=pltpu.VMEM)
    hbm = pl.BlockSpec(memory_space=pltpu.HBM)
    f32 = jnp.float32
    return pl.pallas_call(
        kernel,
        out_shape=(pltpu.VMEM(phase_noise.shape, f32), pltpu.VMEM(potentials.shape, f32)),
        in_specs=[hbm] * 4,
        out_specs=(vmem, vmem),
        scratch_shapes=[
            pltpu.VMEM(labels.shape, jnp.int32),
            pltpu.VMEM(phase_noise.shape, f32),
            pltpu.VMEM(potentials.shape, f32),
            pltpu.SMEM(frame_shift.shape, jnp.int32),
            pltpu.SemaphoreType.DMA((4,)),
            pltpu.VMEM((STEPS // 2, 5, rows, ny, nl), f32),
            pltpu.VMEM((STEPS + 1, 5, rows + 4, 4, ny, nl), f32),
            pltpu.VMEM((STEPS, 2, 5, rows, ny, nl), f32),
            pltpu.VMEM((STEPS, 2, 4, ny, nl), f32),
            pltpu.VMEM((STEPS, 2, 4, ny, nl), f32),
            pltpu.VMEM((STEPS, 2, 4, ny, nl), f32),
            pltpu.VMEM((STEPS, 2, 4, ny, nl), f32),
            pltpu.VMEM((STEPS, 2, ny, nl), f32),
            pltpu.VMEM((STEPS, 2, ny, nl), f32),
            pltpu.VMEM((STEPS, 4, ny, nl), f32),
            pltpu.VMEM((STEPS, 4, ny, nl), f32),
            pltpu.VMEM((STEPS, 4, ny, nl), f32),
            pltpu.VMEM((STEPS, 4, ny, nl), f32),
            pltpu.SemaphoreType.DMA((STEPS, 20)),
            pltpu.SemaphoreType.DMA((STEPS, 20)),
        ],
        compiler_params=pltpu.CompilerParams(collective_id=0, has_side_effects=True),
        name="eutectic",
    )(labels, phase_noise, potentials, frame_shift)


def solution(mesh):
    placed = (P("gx", "gy"), P(None, "gx", "gy", "gz"), P(None, "gx", "gy", "gz"), P())
    return jax.shard_map(
        on_device,
        mesh=mesh,
        in_specs=placed,
        out_specs=(P(None, "gx", "gy", "gz"), P(None, "gx", "gy", "gz")),
        check_vma=False,
    )
```

```python
import functools
import math

import jax
import jax.numpy as jnp
from jax import lax
from jax.experimental import pallas as pl
from jax.experimental.pallas import tpu as pltpu
from jax.sharding import PartitionSpec as P

MESH = pl.DeviceIdType.MESH
STEPS = 4

interface_width = 4.0
time_step = 0.12
obstacle_coef = 16.0 / (math.pi * math.pi)
normal_floor = 0.25
surface_table = [
    [0.0, 1.0, 1.2, 0.9],
    [1.0, 0.0, 1.1, 1.0],
    [1.2, 1.1, 0.0, 0.8],
    [0.9, 1.0, 0.8, 0.0],
]
compositions = [[0.8, 0.1], [0.1, 0.8], [0.1, 0.1], [0.33, 0.33]]
latent_heat = [1.0, 0.9, 1.1, 0.0]
trapping_coef = math.pi * 4.0 / 4.0
undercool_span = 2.0

OWN, YH, ZH, YZ = 0, 1, 2, 3


def phase_update(center, nb, m, theta):
    lap = []
    for a in range(3):
        total = (nb[0][0][a] + nb[0][1][a]) + (nb[1][0][a] + nb[1][1][a])
        total = total + (nb[2][0][a] + nb[2][1][a])
        lap.append(total - 6.0 * center[a])
    lap.append(-(lap[0] + lap[1] + lap[2]))
    p = list(center) + [1.0 - (center[0] + center[1] + center[2])]

    def weigh(f, a):
        terms = [f[b] if surface_table[a][b] == 1.0 else surface_table[a][b] * f[b] for b in range(4) if b != a]
        return terms[0] + terms[1] + terms[2]

    drive = []
    for a in range(4):
        gp = weigh(p, a)
        gl = weigh(lap, a)
        v = gp * (obstacle_coef / interface_width - interface_width * lap[a]) + (interface_width * p[a]) * gl
        v = v - (compositions[a][0] * m[0] + compositions[a][1] * m[1])
        if latent_heat[a]:
            v = v + latent_heat[a] * theta
        drive.append(v)
    mean = 0.25 * ((drive[0] + drive[1]) + (drive[2] + drive[3]))
    q = [jnp.clip(p[a] - (time_step / interface_width) * (drive[a] - mean), 0.0, 1.0) for a in range(4)]
    inv = 1.0 / ((q[0] + q[1]) + (q[2] + q[3]))
    new = [q[a] * inv for a in range(4)]
    rate = [(new[a] - p[a]) * (1.0 / time_step) for a in range(4)]
    return p, new, rate


def carried_part(p, rate, nb):
    p3 = p[3] * 4.0
    carried, slopes = [], []
    for a in range(3):
        g = [0.5 * (nb[d][1][a] - nb[d][0][a]) for d in range(3)]
        square = g[0] * g[0] + g[1] * g[1] + g[2] * g[2]
        inv = lax.rsqrt(jnp.maximum(square, normal_floor * normal_floor))
        carried.append(p[a] * p3 * rate[a] * inv)
        slopes.append(g)
    return carried, slopes


def current(carried, slopes, d):
    out = []
    for k in range(2):
        total = None
        for a in range(3):
            term = (-trapping_coef * (compositions[3][k] - compositions[a][k])) * (carried[a] * slopes[a][d])
            total = term if total is None else total + term
        out.append(total)
    return out


def kernel(labels_hbm, noise_hbm, pot_hbm, shift_hbm, phase_out, pot_out,
           labels_ref, noise_ref, pot_ref, shift_ref, in_sem,
           S, W, zrcv, ysnd, yrcv, yzsnd, yzrcv, xzsnd, xzrcv, csnd, crcv, czsnd, czrcv, send_sem, recv_sem):
    fetches = [
        pltpu.make_async_copy(src, dst, in_sem.at[n])
        for n, (src, dst) in enumerate(
            ((labels_hbm, labels_ref), (noise_hbm, noise_ref), (pot_hbm, pot_ref), (shift_hbm, shift_ref))
        )
    ]
    for fetch in fetches:
        fetch.start()
    rows, ny, nl = noise_ref.shape[1:]
    gx, gy, gz = lax.axis_index("gx"), lax.axis_index("gy"), lax.axis_index("gz")
    nx_dev, ny_dev, nz_dev = lax.axis_size("gx"), lax.axis_size("gy"), lax.axis_size("gz")

    def near(index, count, step):
        return lax.rem(index + (count + step), count)

    xs = {-1: near(gx, nx_dev, -1), 1: near(gx, nx_dev, 1)}
    ys = {-1: near(gy, ny_dev, -1), 1: near(gy, ny_dev, 1)}
    zs = {-1: near(gz, nz_dev, -1), 1: near(gz, nz_dev, 1)}
    corners = [(-1, -1), (-1, 1), (1, -1), (1, 1)]
    targets = [{"gx": xs[i], "gy": ys[j]} for i, j in corners]
    targets += [{"gx": xs[-1]}, {"gx": xs[1]}, {"gy": ys[-1]}, {"gy": ys[1]}, {"gz": zs[-1]}, {"gz": zs[1]}]

    barrier = pltpu.get_barrier_semaphore()
    for target in targets:
        pl.semaphore_signal(barrier, inc=1, device_id=target, device_id_type=MESH)

    lane = lax.broadcasted_iota(jnp.int32, (ny, nl), 1)
    row = lax.broadcasted_iota(jnp.int32, (ny, nl), 0)
    lower = gz == 0
    upper = gz == nz_dev - 1
    total_planes = nl * nz_dev
    front = total_planes // 2
    zown = gz * nl + lane
    zhalo = jnp.where(lane < nl // 2, zown + nl, zown - nl)

    def theta_of(index):
        return undercool_span * (index.astype(jnp.float32) + 0.5 - front) / total_planes

    theta = {OWN: theta_of(zown), ZH: theta_of(zhalo)}
    theta[YH] = theta[OWN]
    solid = zown < front

    def up_y(a, b):
        return pltpu.roll(jnp.where(row == 0, b, a), ny - 1, 0)

    def down_y(a, b):
        return pltpu.roll(jnp.where(row == ny - 1, b, a), 1, 0)

    def up_z(a, b):
        return pltpu.roll(jnp.where(lane == 0, b, a), nl - 1, 1)

    def down_z(a, b):
        return pltpu.roll(jnp.where(lane == nl - 1, b, a), 1, 1)

    for fetch in fetches:
        fetch.wait()
    first_shift, second_shift = shift_ref[0], shift_ref[1]
    lrow = lax.broadcasted_iota(jnp.int32, (ny, ny), 0)
    lcol = lax.broadcasted_iota(jnp.int32, (ny, ny), 1)
    for x in range(rows):
        lab = jnp.broadcast_to(labels_ref[x : x + 1, :].astype(jnp.float32), (ny, ny))
        lab = jnp.sum(jnp.where(lrow == lcol, lab, 0.0), axis=1, keepdims=True)
        lab = jnp.broadcast_to(lab, (ny, nl))
        init = []
        for a in range(3):
            init.append(noise_ref[a, x] + jnp.where((lab == float(a)) & solid, 1.0, 0.0))
        init.append(noise_ref[3, x] + jnp.where(solid, 0.0, 1.0))
        inv = 1.0 / ((init[0] + init[1]) + (init[2] + init[3]))
        for a in range(3):
            W[0, a, x + 2, OWN] = init[a] * inv
        for k in range(2):
            W[0, 3 + k, x + 2, OWN] = pot_ref[k, x]

    pl.semaphore_wait(barrier, len(targets))

    def step(t, shifted, store):
        def copy(src, dst, n, target):
            return pltpu.make_async_remote_copy(
                src_ref=src, dst_ref=dst, send_sem=send_sem.at[t, n], recv_sem=recv_sem.at[t, n],
                device_id=target, device_id_type=MESH,
            )

        block = S.at[t // 2] if shifted else W.at[t, pl.ds(0, 5), pl.ds(2, rows), OWN]
        zcopies = [
            copy(block, zrcv.at[t, 0], 0, {"gz": zs[1]}),
            copy(block, zrcv.at[t, 1], 1, {"gz": zs[-1]}),
        ]
        for c in zcopies:
            c.start()

        copies = []

        def launch(c):
            c.start()
            copies.append(c)

        def pack_own(x, f, own):
            if f < 3:
                ysnd[t, 0, f, 2 * x : 2 * x + 2, :] = own[0:2]
                ysnd[t, 1, f, 2 * x : 2 * x + 2, :] = own[ny - 2 : ny]
                for n, (i, j) in enumerate(corners):
                    if x == (0 if i < 0 else rows - 1):
                        csnd[t, n, f : f + 1, :] = own[0:1] if j < 0 else own[ny - 1 : ny]
            else:
                at = (f - 3) * rows + x
                ysnd[t, 0, 3, at : at + 1, :] = own[0:1]
                ysnd[t, 1, 3, at : at + 1, :] = own[ny - 1 : ny]

        def send_own():
            low, high = (2, rows + 2), (rows, 0)
            for side, (src, dst) in ((-1, low), (1, high)):
                base = 6 + (0 if side < 0 else 2)
                edge_src = 2 if side < 0 else rows + 1
                edge_dst = rows + 2 if side < 0 else 1
                target = {"gx": xs[side]}
                faces = S.at[t // 2, pl.ds(0, 3), pl.ds(src - 2, 2)] if shifted else W.at[t, pl.ds(0, 3), pl.ds(src, 2), OWN]
                chem = S.at[t // 2, pl.ds(3, 2), edge_src - 2] if shifted else W.at[t, pl.ds(3, 2), edge_src, OWN]
                launch(copy(faces, W.at[t, pl.ds(0, 3), pl.ds(dst, 2), OWN], base, target))
                launch(copy(chem, W.at[t, pl.ds(3, 2), edge_dst, OWN], base + 1, target))

        def send_y():
            for n, (i, j) in enumerate(corners):
                launch(copy(csnd.at[t, n], crcv.at[t, n], 2 + n, {"gx": xs[i], "gy": ys[j]}))
            launch(copy(ysnd.at[t, 0], yrcv.at[t, 0], 10, {"gy": ys[-1]}))
            launch(copy(ysnd.at[t, 1], yrcv.at[t, 1], 11, {"gy": ys[1]}))

        def source(x, f):
            return S[t // 2, f, x] if shifted else W[t, f, x + 2, OWN]

        for x in range(rows):
            for f in range(5):
                pack_own(x, f, source(x, f))
        send_y()
        send_own()
        for c in zcopies:
            c.wait_recv()

        def clamp(own, halo):
            first = jnp.broadcast_to(own[:, 0:1], (ny, nl))
            last = jnp.broadcast_to(own[:, nl - 1 : nl], (ny, nl))
            halo = jnp.where(upper & (lane < nl // 2), last, halo)
            return jnp.where(lower & (lane >= nl // 2), first, halo)

        if shifted:
            amount = jnp.where(t == 1, first_shift, second_shift)
            shift = jnp.full((ny, nl), amount, jnp.int32)

        def moved(own, halo):
            keep = lane < nl - shift
            own, halo = pltpu.roll(own, nl - amount, 1), pltpu.roll(halo, nl - amount, 1)
            own, halo = jnp.where(keep, own, halo), jnp.where(keep, halo, own)
            return own, halo

        def roll_by(value, by):
            return pltpu.roll(value, by % nl, 1) if by % nl else value

        packed = [None, None]

        def pack_edge(side, at, width, low, value):
            inside = (lane >= width * at - low) & (lane < width * (at + 1) - low)
            if at == 0:
                packed[side] = value
            else:
                packed[side] = jnp.where(inside, roll_by(value, width * at), packed[side])

        for f in range(5):
            for x in range(rows):
                if shifted:
                    above = jnp.where(upper, 0.0, zrcv[t, 1, f, x])
                    if f < 3:
                        yzsnd[t, 0, f, 2 * x : 2 * x + 2, :] = above[0:2]
                        yzsnd[t, 1, f, 2 * x : 2 * x + 2, :] = above[ny - 2 : ny]
                        for n, (i, j) in enumerate(corners):
                            if x == (0 if i < 0 else rows - 1):
                                czsnd[t, n, f : f + 1, :] = above[0:1] if j < 0 else above[ny - 1 : ny]
                        if x < 2:
                            pack_edge(0, 2 * f + x, 16, 0, above)
                        if x >= rows - 2 and (f or x == rows - 1):
                            pack_edge(1, 2 * f + (rows - 1 - x), 16, 0, above)
                    else:
                        at = (f - 3) * rows + x
                        yzsnd[t, 0, 3, at : at + 1, :] = above[0:1]
                        yzsnd[t, 1, 3, at : at + 1, :] = above[ny - 1 : ny]
                        if x == 0:
                            pack_edge(0, 6 + f - 3, 16, 0, above)
                        if x == rows - 1:
                            pack_edge(1, 6 + f - 3, 16, 0, above)
                    if f == 0 and x == rows - 1:
                        second = jnp.where(upper, 0.0, zrcv[t, 1, 0, rows - 2])
                        pack_edge(1, 1, 16, 0, second)
                else:
                    own = source(x, f)
                    halo = clamp(own, jnp.where(lane < nl // 2, zrcv[t, 1, f, x], zrcv[t, 0, f, x]))
                    W[t, f, x + 2, ZH] = halo
                    if f < 3:
                        yzsnd[t, 0, f, 2 * x : 2 * x + 1, :] = halo[0:1]
                        yzsnd[t, 1, f, 2 * x + 1 : 2 * x + 2, :] = halo[ny - 1 : ny]
                        if x == 0:
                            pack_edge(0, f, 8, 1, halo)
                        if x == rows - 1:
                            pack_edge(1, f, 8, 1, halo)
        xzsnd[t, 0] = packed[0]
        xzsnd[t, 1] = packed[1]
        if shifted:
            for n, (i, j) in enumerate(corners):
                launch(copy(czsnd.at[t, n], czrcv.at[t, n], 16 + n, {"gx": xs[i], "gy": ys[j]}))
        launch(copy(yzsnd.at[t, 0], yzrcv.at[t, 0], 14, {"gy": ys[-1]}))
        launch(copy(yzsnd.at[t, 1], yzrcv.at[t, 1], 15, {"gy": ys[1]}))
        launch(copy(xzsnd.at[t, 0], xzrcv.at[t, 0], 12, {"gx": xs[-1]}))
        launch(copy(xzsnd.at[t, 1], xzrcv.at[t, 1], 13, {"gx": xs[1]}))
        if shifted:
            for x in range(rows):
                for f in range(5):
                    above = jnp.where(upper, 0.0, zrcv[t, 1, f, x])
                    halo = jnp.where(lane < nl // 2, above, zrcv[t, 0, f, x])
                    own, halo = moved(source(x, f), halo)
                    W[t, f, x + 2, OWN] = own
                    W[t, f, x + 2, ZH] = clamp(own, halo)
        for c in copies:
            c.wait_recv()

        for slot, edge, outer in ((0, rows + 2, rows + 3), (1, 1, 0)):
            halo_pack = xzrcv[t, slot]
            for f in range(5):
                if not shifted:
                    if f < 3:
                        W[t, f, edge, ZH] = roll_by(halo_pack, nl - 8 * f)
                    continue
                at = 2 * f if f < 3 else 6 + f - 3
                own, halo = moved(W[t, f, edge, OWN], roll_by(halo_pack, nl - 16 * at))
                W[t, f, edge, OWN] = own
                if f < 3:
                    W[t, f, edge, ZH] = clamp(own, halo)
                    W[t, f, outer, OWN] = moved(W[t, f, outer, OWN], roll_by(halo_pack, nl - 16 * (at + 1)))[0]

        for f in range(4):
            faces = []
            for slot in range(2):
                own, halo = yrcv[t, slot, f], yzrcv[t, slot, f]
                if shifted:
                    own, halo = moved(own, halo)
                    if f < 3:
                        halo = clamp(own, halo)
                faces.append((own, halo))
            for x in range(rows):
                if f < 3:
                    W[t, f, x + 2, YH, 0:2, :] = faces[0][0][2 * x : 2 * x + 2]
                    W[t, f, x + 2, YH, ny - 2 : ny, :] = faces[1][0][2 * x : 2 * x + 2]
                    W[t, f, x + 2, YZ, 0:1, :] = faces[0][1][2 * x : 2 * x + 1]
                    W[t, f, x + 2, YZ, ny - 1 : ny, :] = faces[1][1][2 * x + 1 : 2 * x + 2]
                else:
                    for k in range(2):
                        at = k * rows + x
                        W[t, 3 + k, x + 2, YH, 0:1, :] = faces[0][0][at : at + 1]
                        W[t, 3 + k, x + 2, YH, ny - 1 : ny, :] = faces[1][0][at : at + 1]
        for n, (i, j) in enumerate(corners):
            xdst = rows + 2 if i < 0 else 1
            ydst = 0 if j < 0 else ny - 1
            own = crcv[t, n]
            if shifted:
                own, _ = moved(own, czrcv[t, n])
            for f in range(3):
                W[t, f, xdst, YH, ydst : ydst + 1, :] = own[f : f + 1]

        def field(x, q, fs=(0, 1, 2)):
            return [W[t, f, x, q] for f in fs]

        partner_y = {OWN: YH, YH: OWN, ZH: YZ}
        partner_z = {OWN: ZH, ZH: OWN, YH: YZ}

        def neighbours(x, q, fs=(0, 1, 2), with_x=True):
            c = field(x, q, fs)
            py = field(x, partner_y[q], fs)
            pz = field(x, partner_z[q], fs)
            n = len(fs)
            return c, [
                (field(x - 1, q, fs), field(x + 1, q, fs)),
                ([down_y(c[a], py[a]) for a in range(n)], [up_y(c[a], py[a]) for a in range(n)]),
                ([down_z(c[a], pz[a]) for a in range(n)], [up_z(c[a], pz[a]) for a in range(n)]),
            ]

        jx = {}
        partial = {}
        for x in range(1, rows + 3):
            inside = 2 <= x < rows + 2
            m = field(x, OWN, (3, 4))
            c, nb = neighbours(x, OWN)
            p, new, rate = phase_update(c, nb, m, theta[OWN])
            carried, slopes = carried_part(p, rate, nb)
            jx[x] = current(carried, slopes, 0)
            if inside:
                for a in range(3):
                    store(a, x - 2, new[a])
                phase_out[3, x - 2] = new[3]
                _, mb = neighbours(x, OWN, (3, 4))
                diff = [None, None]
                s = (c[0] + c[1]) + c[2]
                for d in range(3):
                    for side in range(2):
                        around = nb[d][side]
                        mob = 1.0 - 0.45 * (((around[0] + around[1]) + around[2]) + s)
                        for k in range(2):
                            flow = mob * (mb[d][side][k] - m[k])
                            diff[k] = flow if diff[k] is None else diff[k] + flow
                for k in range(2):
                    for a in range(4):
                        diff[k] = diff[k] - compositions[a][k] * rate[a]
                jy = current(carried, slopes, 1)
                jz = current(carried, slopes, 2)
                cb, nbb = neighbours(x, YH)
                pb, _, rb = phase_update(cb, nbb, field(x, YH, (3, 4)), theta[YH])
                jyb = current(*carried_part(pb, rb, nbb), 1)
                cz, nbz = neighbours(x, ZH)
                pz, _, rz = phase_update(cz, nbz, field(x, ZH, (3, 4)), theta[ZH])
                jzb = current(*carried_part(pz, rz, nbz), 2)
                for k in range(2):
                    dy = up_y(jy[k], jyb[k]) - down_y(jy[k], jyb[k])
                    above = jnp.where(upper & (lane == nl - 1), jz[k], up_z(jz[k], jzb[k]))
                    below = jnp.where(lower & (lane == 0), jz[k], down_z(jz[k], jzb[k]))
                    diff[k] = diff[k] - 0.5 * (dy + (above - below))
                partial[x] = (m, diff)
            if x >= 3:
                at = x - 1
                if 2 <= at < rows + 2:
                    m_at, diff_at = partial.pop(at)
                    for k in range(2):
                        total = diff_at[k] - 0.5 * (jx[at + 1][k] - jx[at - 1][k])
                        store(3 + k, at - 2, m_at[k] + time_step * total)
        for c in zcopies + copies:
            c.wait_send()

    def pair(tt, carry):
        def to_block(f, x, value):
            S[tt, f, x] = value

        def to_window(f, x, value):
            W[2 * tt + 2, f, x + 2, OWN] = value

        step(2 * tt, False, to_block)
        step(2 * tt + 1, True, to_window)
        return carry

    lax.fori_loop(0, STEPS // 2, pair, 0)
    for x in range(rows):
        for a in range(3):
            phase_out[a, x] = W[STEPS, a, x + 2, OWN]
        for k in range(2):
            pot_out[k, x] = W[STEPS, 3 + k, x + 2, OWN]


def on_device(labels, phase_noise, potentials, frame_shift):
    _, rows, ny, nl = phase_noise.shape
    vmem = pl.BlockSpec(memory_space=pltpu.VMEM)
    hbm = pl.BlockSpec(memory_space=pltpu.HBM)
    f32 = jnp.float32
    return pl.pallas_call(
        kernel,
        out_shape=(pltpu.VMEM(phase_noise.shape, f32), pltpu.VMEM(potentials.shape, f32)),
        in_specs=[hbm] * 4,
        out_specs=(vmem, vmem),
        scratch_shapes=[
            pltpu.VMEM(labels.shape, jnp.int32),
            pltpu.VMEM(phase_noise.shape, f32),
            pltpu.VMEM(potentials.shape, f32),
            pltpu.SMEM(frame_shift.shape, jnp.int32),
            pltpu.SemaphoreType.DMA((4,)),
            pltpu.VMEM((STEPS // 2, 5, rows, ny, nl), f32),
            pltpu.VMEM((STEPS + 1, 5, rows + 4, 4, ny, nl), f32),
            pltpu.VMEM((STEPS, 2, 5, rows, ny, nl), f32),
            pltpu.VMEM((STEPS, 2, 4, ny, nl), f32),
            pltpu.VMEM((STEPS, 2, 4, ny, nl), f32),
            pltpu.VMEM((STEPS, 2, 4, ny, nl), f32),
            pltpu.VMEM((STEPS, 2, 4, ny, nl), f32),
            pltpu.VMEM((STEPS, 2, ny, nl), f32),
            pltpu.VMEM((STEPS, 2, ny, nl), f32),
            pltpu.VMEM((STEPS, 4, ny, nl), f32),
            pltpu.VMEM((STEPS, 4, ny, nl), f32),
            pltpu.VMEM((STEPS, 4, ny, nl), f32),
            pltpu.VMEM((STEPS, 4, ny, nl), f32),
            pltpu.SemaphoreType.DMA((STEPS, 20)),
            pltpu.SemaphoreType.DMA((STEPS, 20)),
        ],
        compiler_params=pltpu.CompilerParams(collective_id=0, has_side_effects=True),
        name="eutectic",
    )(labels, phase_noise, potentials, frame_shift)


def solution(mesh):
    placed = (P("gx", "gy"), P(None, "gx", "gy", "gz"), P(None, "gx", "gy", "gz"), P())
    return jax.shard_map(
        on_device,
        mesh=mesh,
        in_specs=placed,
        out_specs=(P(None, "gx", "gy", "gz"), P(None, "gx", "gy", "gz")),
        check_vma=False,
    )
```
